128 devices in a mesh: keys: 32 (over y, z, core), view: 4 (over x).
Axes of the slice: x: 4, y: 4, z: 4, core: 2. Of those that a mesh axis runs over, the one named last changes fastest.
Arguments:
- key_slot: int32 [16384], replicated, may hold values from 0 to 16383, as said below
- a_slot: int32 [524288], P(('keys', 'view')), may hold values from 0 to 511
- a_group: int32 [524288], P(('keys', 'view')), may hold values from 0 to 4095
- a_weight: int32 [524288], P(('keys', 'view')), may hold values from 1 to 3
- a_payload: bfloat16 [524288, 256], P(('keys', 'view')), may hold values from -1.1953125 to 1.1953125
- b_slot: int32 [524288], P(('keys', 'view')), may hold values from 0 to 511
- b_weight: int32 [524288], P(('keys', 'view')), may hold values from 1 to 3
- b_payload: bfloat16 [524288, 256], P(('keys', 'view')), may hold values from -0.59765625 to 0.59765625
- da_key: int32 [131072], P(('keys', 'view')), may hold values from 0 to 16383, as said below
- da_group: int32 [131072], P(('keys', 'view')), may hold values from 0 to 4095
- da_mult: int32 [131072], P(('keys', 'view')), may hold values from -1 to 1, as said below
- da_payload: bfloat16 [131072, 256], P(('keys', 'view')), may hold values from -1.796875 to 1.796875
- da_count: int32 [128], P(('keys', 'view')), may hold values from 768 to 1024, as said below
- db_key: int32 [131072], P(('keys', 'view')), may hold values from 0 to 16383, as said below
- db_mult: int32 [131072], P(('keys', 'view')), may hold values from -1 to 1, as said below
- db_payload: bfloat16 [131072, 256], P(('keys', 'view')), may hold values from -1.1953125 to 1.1953125
- db_count: int32 [128], P(('keys', 'view')), may hold values from 768 to 1024, as said below
Outputs:
- view_delta: float32 [4096, 256], P(('keys', 'view'))
The draws below stay inside these ranges and needn't reach their ends.
Inputs may be any that keep to these rules, and one draw needn't show every extreme that they name: `key_slot`: A permutation of 0 to 16383. `da_key`: among the 1024 slots of one device, at most 64 have keys held by one keys index; in every draw one keys index gets exactly 64 live rows from every device. `db_key`: among the 1024 slots of one device, at most 64 have keys held by one keys index; in every draw one keys index gets exactly 64 live rows from every device. `da_mult`: each entry is -1 or 1. `db_mult`: each entry is -1 or 1. `da_count`: some device has all 1024 rows live. `db_count`: some device has all 1024 rows live.
All inputs are finite; a program needn't handle non-finite values.
Results may differ from the reference program's by a relative error of at most 0.0029.
Values may be sent and summed in bfloat16 or wider, within the bound.
A program may use at most 64 MiB of HBM per device.

```python
import jax
import jax.numpy as jnp

D = 256
KEYS_DEV = 512
GROUPS_DEV = 32
A_DEV = 4096
B_DEV = 4096
DELTA_DEV = 1024
CAP = 64
KEYS = 16384
GROUPS = 4096
A_ROWS = 524288
B_ROWS = 524288
DELTA_ROWS = 131072
N_KEYS = 32
N_VIEW = 4


def draw_key_slot(key, part):
    return jax.random.permutation(jax.random.fold_in(key, 11), KEYS).astype(jnp.int32)


def delta_keys(key, salt_value):
    order = draw_key_slot(key, 0)
    inverse = jnp.zeros((KEYS,), jnp.int32).at[order].set(jnp.arange(KEYS, dtype=jnp.int32))
    base = jax.random.fold_in(key, salt_value)
    hot_owner = jax.random.randint(jax.random.fold_in(base, 1), (), 0, N_KEYS).astype(jnp.int32)
    others = (hot_owner + 1 + jnp.arange(N_KEYS - 1, dtype=jnp.int32)) % N_KEYS
    target_pool = jnp.repeat(others, CAP, total_repeat_length=(N_KEYS - 1) * CAP)
    device_keys = jax.random.split(jax.random.fold_in(base, 2), N_KEYS * N_VIEW)

    def one_device(device_key):
        shuffled = jax.random.permutation(jax.random.fold_in(device_key, 3), target_pool)
        target = jnp.concatenate([jnp.full((CAP,), hot_owner, jnp.int32), shuffled[:DELTA_DEV - CAP]])
        within = jax.random.randint(jax.random.fold_in(device_key, 4), (DELTA_DEV,), 0, KEYS_DEV).astype(jnp.int32)
        return jnp.take(inverse, target * KEYS_DEV + within)
    return jax.vmap(one_device)(device_keys).reshape(-1).astype(jnp.int32)


def delta_signs(key, salt_value):
    picked = jax.random.randint(jax.random.fold_in(key, salt_value), (DELTA_ROWS,), 0, 2)
    return (2 * picked - 1).astype(jnp.int32)


def delta_counts(key, salt_value):
    devices = N_KEYS * N_VIEW
    counts = jax.random.randint(jax.random.fold_in(key, salt_value), (devices,), 3 * DELTA_DEV // 4, DELTA_DEV + 1)
    full_device = jax.random.randint(jax.random.fold_in(key, salt_value + 1), (), 0, devices)
    return counts.at[full_device].set(DELTA_DEV).astype(jnp.int32)


def draw_da_key(key, part):
    return delta_keys(key, 21)


def draw_db_key(key, part):
    return delta_keys(key, 22)


def draw_da_mult(key, part):
    return delta_signs(key, 31)


def draw_db_mult(key, part):
    return delta_signs(key, 32)


def draw_da_count(key, part):
    return delta_counts(key, 41)


def draw_db_count(key, part):
    return delta_counts(key, 51)


def plant(entries, own_key, smallest, high):
    dims = entries.shape
    place = [jax.random.randint(jax.random.fold_in(own_key, axis), (), 0, dims[axis]) for axis in range(len(dims))]
    entries = entries.at[tuple(place)].set(smallest)
    longest = dims.index(max(dims))
    place[longest] = (place[longest] + 1) % dims[longest]
    return entries.at[tuple(place)].set(high)


def block_scale(key, dims, pieces, least, high):
    gain = 1.0
    for axis_at, shards_of in pieces:
        heights = jax.random.uniform(jax.random.fold_in(jax.random.fold_in(key, 6), axis_at), (shards_of,), jnp.float32, least / len(pieces), high / len(pieces))
        gain = gain * jnp.repeat(jnp.exp(heights), dims[axis_at] // shards_of).reshape((-1,) + (1,) * (len(dims) - 1 - axis_at))
    return gain


def scatter_about(key, shape, width, bound, cuts=(), held_as=jnp.bfloat16):
    result = width * jax.random.normal(key, shape, jnp.float32)
    if cuts:
        result = result * block_scale(key, shape, cuts, -0.22, 0.18)
    return jnp.clip(result, -bound, bound).astype(held_as)


def setup_inputs(seed: int = 0) -> dict:
    splits = jax.random.split(jax.random.key(seed), 18)
    key_slot = draw_key_slot(jax.random.fold_in(splits[17], 71), 0)
    a_slot = plant(jax.random.randint(splits[1], (A_ROWS,), 0, KEYS_DEV), jax.random.fold_in(splits[1], 1), 0, KEYS_DEV - 1).astype(jnp.int32)
    a_group = plant(jax.random.randint(splits[2], (A_ROWS,), 0, GROUPS), jax.random.fold_in(splits[2], 1), 0, GROUPS - 1).astype(jnp.int32)
    a_weight = plant(jax.random.randint(splits[3], (A_ROWS,), 1, 4), jax.random.fold_in(splits[3], 1), 1, 3).astype(jnp.int32)
    a_payload = scatter_about(splits[4], (A_ROWS, D), 0.2, 1.1953125, ((0, 128),))
    b_slot = plant(jax.random.randint(splits[5], (B_ROWS,), 0, KEYS_DEV), jax.random.fold_in(splits[5], 1), 0, KEYS_DEV - 1).astype(jnp.int32)
    b_weight = plant(jax.random.randint(splits[6], (B_ROWS,), 1, 4), jax.random.fold_in(splits[6], 1), 1, 3).astype(jnp.int32)
    b_payload = scatter_about(splits[7], (B_ROWS, D), 0.1, 0.59765625, ((0, 128),))
    da_key = draw_da_key(jax.random.fold_in(splits[17], 71), 0)
    da_group = plant(jax.random.randint(splits[9], (DELTA_ROWS,), 0, GROUPS), jax.random.fold_in(splits[9], 1), 0, GROUPS - 1).astype(jnp.int32)
    da_mult = draw_da_mult(jax.random.fold_in(splits[17], 71), 0)
    da_payload = scatter_about(splits[11], (DELTA_ROWS, D), 0.3, 1.796875, ((0, 128),))
    da_count = draw_da_count(jax.random.fold_in(splits[17], 71), 0)
    db_key = draw_db_key(jax.random.fold_in(splits[17], 71), 0)
    db_mult = draw_db_mult(jax.random.fold_in(splits[17], 71), 0)
    db_payload = scatter_about(splits[15], (DELTA_ROWS, D), 0.2, 1.1953125, ((0, 128),))
    db_count = draw_db_count(jax.random.fold_in(splits[17], 71), 0)
    return dict(key_slot=key_slot, a_slot=a_slot, a_group=a_group, a_weight=a_weight, a_payload=a_payload, b_slot=b_slot, b_weight=b_weight, b_payload=b_payload, da_key=da_key, da_group=da_group, da_mult=da_mult, da_payload=da_payload, da_count=da_count, db_key=db_key, db_mult=db_mult, db_payload=db_payload, db_count=db_count)


def reference(key_slot, a_slot, a_group, a_weight, a_payload, b_slot, b_weight, b_payload, da_key, da_group, da_mult, da_payload, da_count, db_key, db_mult, db_payload, db_count):
    devices = N_KEYS * N_VIEW
    total_keys = KEYS_DEV * N_KEYS
    total_groups = GROUPS_DEV * devices

    def owner_slots(local_slot, rows_dev):
        device_index = jnp.arange(local_slot.shape[0], dtype=jnp.int32) // rows_dev
        return (device_index // N_VIEW) * KEYS_DEV + local_slot

    def signed_rows(row_mult, row_count):
        position = jnp.arange(DELTA_DEV * devices, dtype=jnp.int32)
        alive_rows = (position % DELTA_DEV) < jnp.take(row_count, position // DELTA_DEV)
        return (row_mult * alive_rows.astype(jnp.int32)).astype(jnp.float32)

    key_b = jax.ops.segment_sum(b_weight[:, None].astype(jnp.float32) * b_payload.astype(jnp.float32), owner_slots(b_slot, B_DEV), num_segments=total_keys)
    key_db = jax.ops.segment_sum(signed_rows(db_mult, db_count)[:, None] * db_payload.astype(jnp.float32), jnp.take(key_slot, db_key), num_segments=total_keys)
    a_terms = (a_weight[:, None].astype(jnp.float32) * a_payload.astype(jnp.float32) * jnp.take(key_db, owner_slots(a_slot, A_DEV), axis=0)).astype(jnp.bfloat16)
    whole_table = key_b + key_db
    delta_terms = (signed_rows(da_mult, da_count)[:, None] * da_payload.astype(jnp.float32) * jnp.take(whole_table, jnp.take(key_slot, da_key), axis=0)).astype(jnp.bfloat16)
    view_delta = jax.ops.segment_sum(a_terms.astype(jnp.float32), a_group, num_segments=total_groups)
    view_delta = view_delta + jax.ops.segment_sum(delta_terms.astype(jnp.float32), da_group, num_segments=total_groups)
    return view_delta
```

```python
import functools

import jax
import jax.numpy as jnp
from jax import lax
from jax.experimental import pallas as pl
from jax.experimental.pallas import tpu as pltpu
from jax.sharding import PartitionSpec as P

MESH = pl.DeviceIdType.MESH
F32, BF16, I32 = jnp.float32, jnp.bfloat16, jnp.int32
D = 256
KEYS_DEV = 512
GROUPS_DEV = 32
ROWS = 4096
DELTA = 1024
CAP = 64
OWNERS = 32
VIEWS = 4
LANES = 128
PEERS = 64
HALF = 2048


def iota(shape, dim):
    return lax.broadcasted_iota(I32, shape, dim)


def dot(a, b):
    return jnp.dot(a, b, preferred_element_type=F32)


def one_hot(rows, height, base, values=None):
    at = iota((height, LANES), 0)
    parts = []
    for n, row in enumerate(rows):
        value = 1.0 if values is None else values[n]
        parts.append(jnp.where(at == row - base, value, 0.0).astype(BF16))
    return jnp.concatenate(parts, axis=1)


def split_rows(ref):
    return [ref[s : s + 1, :] for s in range(ref.shape[0])]


def places(table, key_ref, count):
    keys = split_rows(key_ref)
    at = iota((LANES, LANES), 0)
    hits = jnp.concatenate(
        [jnp.where(at == (k >> 7), 1.0, 0.0).astype(BF16) for k in keys], axis=1
    )
    found = dot(table, hits)
    slots, owners, lives, marks = [], [], [], []
    lane = iota((1, LANES), 1)
    owner_at = iota((OWNERS, LANES), 0)
    for s, k in enumerate(keys):
        cut = slice(s * LANES, (s + 1) * LANES)
        value = found[:LANES, cut] * 128.0 + found[LANES:, cut]
        slot = jnp.sum(jnp.where(at == (k & 127), value, 0.0), axis=0, keepdims=True).astype(I32)
        live = lane + s * LANES < count
        owner = jnp.where(live, slot >> 9, -1)
        slots.append(slot & (KEYS_DEV - 1))
        owners.append(owner)
        lives.append(live)
        marks.append(jnp.where(owner_at == owner, 1.0, 0.0))
    stacked = jnp.concatenate(marks, axis=0).astype(BF16)
    col = iota((LANES, 2 * LANES), 1)
    before = jnp.where((iota((LANES, 2 * LANES), 0) < col) | (col >= LANES), 1.0, 0.0).astype(BF16)
    counts = dot(stacked, before)
    carry = jnp.zeros((OWNERS, LANES), F32)
    spots = []
    for s in range(len(keys)):
        cut = slice(s * OWNERS, (s + 1) * OWNERS)
        rank = jnp.sum(marks[s] * (counts[cut, :LANES] + carry), axis=0, keepdims=True).astype(I32)
        spots.append(jnp.where(lives[s], owners[s] * CAP + rank, -1))
        carry = carry + counts[cut, LANES:]
    return slots, spots


def pack_kernel(
    key_slot, da_key, da_group, da_mult, db_key, db_mult, da_count, db_count, da_rows, db_rows,
    da_out, db_out, info_out, spot_ref, sign_ref, info_ref,
):
    whole = key_slot[...]
    high = (whole >> 7).astype(F32).T
    low = (whole & 127).astype(F32).T
    table = jnp.concatenate([high, low], axis=0).astype(BF16)
    for r, (key_ref, mult_ref, count_ref) in enumerate(
        ((db_key, db_mult, db_count), (da_key, da_mult, da_count))
    ):
        slots, spots = places(table, key_ref, count_ref[0])
        for s in range(8):
            cut = slice(s * LANES, (s + 1) * LANES)
            spot_ref[8 * r + s : 8 * r + s + 1, :] = spots[s]
            sign_ref[8 * r + s : 8 * r + s + 1, :] = mult_ref[s : s + 1, :].astype(F32)
            group = da_group[s : s + 1, :]
            rows = [slots[s] >> 4, slots[s] & 15, group >> 6, group & 63]
            zero = jnp.zeros((4, LANES), F32)
            info_ref[r, :, cut] = jnp.concatenate(
                [row.astype(F32) for row in rows] + [zero], axis=0
            ).astype(BF16)

    def chunk(c, carry):
        base = c * 256
        notes = []
        for r, (rows, out) in enumerate(((db_rows, db_out), (da_rows, da_out))):
            spots = [spot_ref[8 * r + s : 8 * r + s + 1, :] for s in range(8)]
            signs = [sign_ref[8 * r + s : 8 * r + s + 1, :] for s in range(8)]
            pick = one_hot(spots, 256, base, signs)
            out[pl.ds(pl.multiple_of(base, 256), 256), :] = dot(pick, rows[...]).astype(BF16)
            notes.append(
                jnp.abs(
                    lax.dot_general(
                        info_ref[r], pick, (((1,), (1,)), ((), ())), preferred_element_type=F32
                    )
                )
            )
        b, a = notes
        rows = jnp.concatenate(
            [
                b[0:1] * 16.0 + b[1:2],
                a[0:1] * 16.0 + a[1:2],
                a[2:3] * 64.0 + a[3:4],
                jnp.zeros((5, 256), F32),
            ],
            axis=0,
        )
        first = iota((8, LANES), 1) < CAP
        for j in range(4):
            v = rows[:, (j // 2) * LANES : (j // 2 + 1) * LANES]
            turned = pltpu.roll(v, CAP, 1)
            kept = jnp.where(first, v, turned) if j % 2 == 0 else jnp.where(first, turned, v)
            info_out[4 * c + j] = kept.astype(I32)
        return carry

    lax.fori_loop(0, 8, chunk, 0)


def wait_bytes(ref, sem):
    pltpu.make_async_copy(ref, ref, sem).wait()


def main_kernel(
    db_send, da_send, info_send, b_rows, b_slot, b_weight, a_rows, a_slot, a_weight, a_group,
    out, db_recv, da_recv, info_recv, part_b, part_db, quarter_b, quarter_db, got_b, got_db,
    full_b, full_db, pick, pick_d, table_hl, table_w, terms, spots, near_send, near_recv,
    far_send, far_recv, own, sems, near_sems,
):
    k, x = lax.axis_index("keys"), lax.axis_index("view")
    core = lax.rem(k, 2)
    partner = k + 1 - 2 * core
    seat = (k // 2) * VIEWS + x

    def peer(j):
        t = lax.rem(seat + j, PEERS)
        return {"keys": (t // VIEWS) * 2 + core, "view": lax.rem(t, VIEWS)}

    def send(src, dst, sem_s, sem_r, device):
        return pltpu.make_async_remote_copy(
            src_ref=src, dst_ref=dst, send_sem=sem_s, recv_sem=sem_r, device_id=device,
            device_id_type=MESH,
        )

    barrier = pltpu.get_barrier_semaphore()

    def greet_same(j, carry):
        pl.semaphore_signal(barrier, inc=1, device_id=peer(j), device_id_type=MESH)
        return carry

    def greet_other(j, carry):
        to = {"keys": lax.rem(k + 2 * j + 1, OWNERS), "view": x}
        pl.semaphore_signal(barrier, inc=1, device_id=to, device_id_type=MESH)
        return carry

    lax.fori_loop(1, PEERS, greet_same, 0)
    lax.fori_loop(0, OWNERS // 2, greet_other, 0)
    pl.semaphore_wait(barrier, PEERS - 1 + OWNERS // 2)

    def to_owner(j, carry):
        owner = lax.rem(k + j, OWNERS)
        to = {"keys": owner, "view": x}
        send(info_send.at[owner], info_recv.at[OWNERS - j], sems.at[0], sems.at[1], to).start()
        send(db_send.at[owner], db_recv.at[OWNERS - j], sems.at[2], sems.at[3], to).start()
        return carry

    lax.fori_loop(1, OWNERS, to_owner, 0)

    def to_owner_a(j, carry):
        owner = lax.rem(k + j, OWNERS)
        to = {"keys": owner, "view": x}
        send(da_send.at[owner], da_recv.at[OWNERS - j], sems.at[4], sems.at[5], to).start()
        return carry

    lax.fori_loop(1, OWNERS, to_owner_a, 0)
    info_recv[0] = info_send[k]
    db_recv[0] = db_send[k]
    da_recv[0] = da_send[k]

    for m in range(2):
        acc = jnp.zeros((256, D), F32)
        for p in range(8):
            rows = [b_slot[4 * p + s : 4 * p + s + 1, :] for s in range(4)]
            values = [b_weight[4 * p + s : 4 * p + s + 1, :].astype(F32) for s in range(4)]
            acc = acc + dot(one_hot(rows, 256, 256 * m, values), b_rows[512 * p : 512 * (p + 1), :])
        part_b[256 * m : 256 * (m + 1), :] = acc

    def quarter(at):
        return pl.ds(pl.multiple_of(at * 128, 128), 128)

    def across(part, got, s):
        for j in range(1, VIEWS):
            to = lax.rem(x + j, VIEWS)
            send(
                part.at[quarter(to)], got.at[j - 1], sems.at[s], sems.at[s + 1],
                {"keys": k, "view": to},
            ).start()

    def all_quarters(mine, full, s):
        for j in range(1, VIEWS):
            to = lax.rem(x + j, VIEWS)
            send(
                mine, full.at[quarter(x)], sems.at[s], sems.at[s + 1], {"keys": k, "view": to}
            ).start()

    across(part_b, got_b, 6)

    at_lane = iota((LANES, LANES), 1)

    def pick_block(j, carry):
        row = a_slot[pl.ds(j, 1), :] + KEYS_DEV * a_weight[pl.ds(j, 1), :]
        cols = jnp.broadcast_to(row.astype(F32), (LANES, LANES)).T.astype(I32)
        slot, weight = cols & (KEYS_DEV - 1), (cols >> 9).astype(F32)
        at = pl.ds(pl.multiple_of(j * LANES, LANES), LANES)
        for q in range(4):
            pick[at, q * LANES : (q + 1) * LANES] = jnp.where(
                at_lane + q * LANES == slot, weight, 0.0
            ).astype(BF16)
        return carry

    lax.fori_loop(0, 32, pick_block, 0)

    def place(group):
        device = group >> 5
        seat_g = (device >> 3) * VIEWS + (device & 3)
        other = ((device >> 2) & 1) ^ core
        return other * HALF + ((seat_g - seat) & (PEERS - 1)) * GROUPS_DEV + (group & 31)

    spots[0:32, :] = place(a_group[...])

    wait_bytes(got_b, sems.at[7])
    quarter_b[...] = part_b[quarter(x), :] + got_b[0] + got_b[1] + got_b[2]
    all_quarters(quarter_b, full_b, 8)
    full_b[quarter(x), :] = quarter_b[...]

    wait_bytes(info_recv.at[1:OWNERS], sems.at[1])
    left = iota((1, LANES), 1) < CAP

    def pair(row, n):
        return jnp.where(left, info_recv[2 * n, row : row + 1, :], info_recv[2 * n + 1, row : row + 1, :])

    for n in range(16):
        spots[32 + n : 33 + n, :] = place(pair(2, n))
        cols = jnp.broadcast_to(pair(1, n).astype(F32), (LANES, LANES)).T.astype(I32)
        for q in range(4):
            pick_d[n * LANES : (n + 1) * LANES, q * LANES : (q + 1) * LANES] = jnp.where(
                at_lane + q * LANES == cols, 1.0, 0.0
            ).astype(BF16)

    wait_bytes(db_recv.at[1:OWNERS], sems.at[3])
    for m in range(2):
        acc = jnp.zeros((256, D), F32)
        for p in range(4):
            rows = [pair(0, 4 * p + s) for s in range(4)]
            blocks = db_recv[8 * p : 8 * (p + 1)].reshape(512, D)
            acc = acc + dot(one_hot(rows, 256, 256 * m), blocks)
        part_db[256 * m : 256 * (m + 1), :] = acc

    across(part_db, got_db, 10)
    wait_bytes(got_db, sems.at[11])
    quarter_db[...] = part_db[quarter(x), :] + got_db[0] + got_db[1] + got_db[2]
    all_quarters(quarter_db, full_db, 12)
    full_db[quarter(x), :] = quarter_db[...]
    wait_bytes(full_b.at[0:384], sems.at[9])
    wait_bytes(full_db.at[0:384], sems.at[13])

    for ref, value in ((table_hl, full_db[...]), (table_w, full_db[...] + full_b[...])):
        top = value.astype(BF16)
        ref[:, :D] = top
        ref[:, D:] = (value - top.astype(F32)).astype(BF16)

    def a_block(j, carry):
        at = pl.ds(pl.multiple_of(j * 256, 256), 256)
        both = dot(pick[at, :], table_hl[...])
        value = (both[:, :D] + both[:, D:]) * a_rows[at, :].astype(F32)
        terms[at, :] = value.astype(BF16)
        return carry

    lax.fori_loop(0, 16, a_block, 0)
    wait_bytes(da_recv.at[1:OWNERS], sems.at[5])

    def d_block(j, carry):
        at = pl.ds(pl.multiple_of(j * 256, 256), 256)
        both = dot(pick_d[at, :], table_w[...])
        rows = da_recv[pl.ds(4 * j, 4)].reshape(256, D)
        value = (both[:, :D] + both[:, D:]) * rows.astype(F32)
        terms[pl.ds(pl.multiple_of(ROWS + j * 256, 256), 256), :] = value.astype(BF16)
        return carry

    lax.fori_loop(0, 8, d_block, 0)

    def summed(base):
        acc = jnp.zeros((256, D), F32)
        for p in range(12):
            rows = [spots[4 * p + s : 4 * p + s + 1, :] for s in range(4)]
            acc = acc + dot(one_hot(rows, 256, base), terms[512 * p : 512 * (p + 1), :])
        return acc

    def to_partner(c):
        near_send[c] = summed(HALF + c * 256)
        send(
            near_send.at[c], near_recv.at[c], near_sems.at[0, c], near_sems.at[1, c],
            {"keys": partner, "view": x},
        ).start()

    to_partner(0)

    def group_chunk(c, carry):
        @pl.when(c < 7)
        def _():
            to_partner(c + 1)

        acc = summed(c * 256)
        wait_bytes(near_recv.at[c], near_sems.at[1, c])
        acc = acc + near_recv[c]

        @pl.when(c == 0)
        def _():
            own[...] = acc[:GROUPS_DEV, :]

        far_send[pl.ds(8 * c, 8)] = acc.astype(BF16).reshape(8, GROUPS_DEV, D)

        def block(j, carry):
            send(
                far_send.at[j], far_recv.at[PEERS - j], sems.at[14], sems.at[15], peer(j)
            ).start()
            return carry

        lax.fori_loop(lax.max(8 * c, 1), 8 * c + 8, block, 0)
        return carry

    lax.fori_loop(0, 8, group_chunk, 0)

    wait_bytes(far_recv.at[1:PEERS], sems.at[15])
    total = own[...]
    for j in range(1, PEERS):
        total = total + far_recv[j].astype(F32)
    out[...] = total

    wait_bytes(info_send.at[1:OWNERS], sems.at[0])
    wait_bytes(db_send.at[1:OWNERS], sems.at[2])
    wait_bytes(da_send.at[1:OWNERS], sems.at[4])
    wait_bytes(part_b.at[0:384], sems.at[6])
    wait_bytes(part_b.at[0:384], sems.at[8])
    wait_bytes(part_db.at[0:384], sems.at[10])
    wait_bytes(part_db.at[0:384], sems.at[12])
    wait_bytes(far_send.at[1:PEERS], sems.at[14])
    for c in range(8):
        wait_bytes(near_send.at[c], near_sems.at[0, c])


def shards(
    key_slot, a_slot, a_group, a_weight, a_payload, b_slot, b_weight, b_payload, da_key, da_group,
    da_mult, da_payload, da_count, db_key, db_mult, db_payload, db_count,
):
    vmem = pl.BlockSpec(memory_space=pltpu.VMEM)
    smem = pl.BlockSpec(memory_space=pltpu.SMEM)

    def lanes(v):
        return v.reshape(-1, LANES)

    db_send, da_send, info = pl.pallas_call(
        pack_kernel_wrapped,
        out_shape=(
            jax.ShapeDtypeStruct((OWNERS * CAP, D), BF16),
            jax.ShapeDtypeStruct((OWNERS * CAP, D), BF16),
            jax.ShapeDtypeStruct((OWNERS, 8, LANES), I32),
        ),
        in_specs=[vmem] * 6 + [smem] * 2 + [vmem] * 2,
        out_specs=(vmem,) * 3,
        scratch_shapes=[
            pltpu.VMEM((16, LANES), I32),
            pltpu.VMEM((16, LANES), F32),
            pltpu.VMEM((2, 8, DELTA), BF16),
        ],
    )(
        lanes(key_slot), lanes(da_key), lanes(da_group), lanes(da_mult), lanes(db_key),
        lanes(db_mult), da_count, db_count, da_payload, db_payload,
    )
    table = (KEYS_DEV, D)
    return pl.pallas_call(
        main_kernel,
        out_shape=jax.ShapeDtypeStruct((GROUPS_DEV, D), F32),
        in_specs=[vmem] * 10,
        out_specs=vmem,
        scratch_shapes=[
            pltpu.VMEM((OWNERS, CAP, D), BF16),
            pltpu.VMEM((OWNERS, CAP, D), BF16),
            pltpu.VMEM((OWNERS, 8, LANES), I32),
            pltpu.VMEM(table, F32),
            pltpu.VMEM(table, F32),
            pltpu.VMEM((128, D), F32),
            pltpu.VMEM((128, D), F32),
            pltpu.VMEM((3, 128, D), F32),
            pltpu.VMEM((3, 128, D), F32),
            pltpu.VMEM(table, F32),
            pltpu.VMEM(table, F32),
            pltpu.VMEM((ROWS, KEYS_DEV), BF16),
            pltpu.VMEM((OWNERS * CAP, KEYS_DEV), BF16),
            pltpu.VMEM((KEYS_DEV, 2 * D), BF16),
            pltpu.VMEM((KEYS_DEV, 2 * D), BF16),
            pltpu.VMEM((ROWS + OWNERS * CAP, D), BF16),
            pltpu.VMEM((48, LANES), I32),
            pltpu.VMEM((8, 256, D), F32),
            pltpu.VMEM((8, 256, D), F32),
            pltpu.VMEM((PEERS, GROUPS_DEV, D), BF16),
            pltpu.VMEM((PEERS, GROUPS_DEV, D), BF16),
            pltpu.VMEM((GROUPS_DEV, D), F32),
            pltpu.SemaphoreType.DMA((16,)),
            pltpu.SemaphoreType.DMA((2, 8)),
        ],
        compiler_params=pltpu.CompilerParams(
            collective_id=0, has_side_effects=True, vmem_limit_bytes=56 * 1024 * 1024
        ),
    )(
        db_send.reshape(OWNERS, CAP, D), da_send.reshape(OWNERS, CAP, D), info, b_payload,
        lanes(b_slot), lanes(b_weight), a_payload, lanes(a_slot), lanes(a_weight), lanes(a_group),
    )


def pack_kernel_wrapped(
    key_slot, da_key, da_group, da_mult, db_key, db_mult, da_count, db_count, da_rows, db_rows,
    db_out, da_out, info_out, spot_ref, sign_ref, info_ref,
):
    pack_kernel(
        key_slot, da_key, da_group, da_mult, db_key, db_mult, da_count, db_count, da_rows, db_rows,
        da_out, db_out, info_out, spot_ref, sign_ref, info_ref,
    )


def solution(mesh):
    rows = P(("keys", "view"))
    wide = P(("keys", "view"), None)
    placed = (
        P(), rows, rows, rows, wide, rows, rows, wide, rows, rows, rows, wide, rows, rows, rows,
        wide, rows,
    )
    return jax.shard_map(
        shards, mesh=mesh, in_specs=placed, out_specs=wide, check_vma=False
    )
```

```python
import jax
import jax.numpy as jnp
from jax import lax
from jax.experimental import pallas as pl
from jax.experimental.pallas import tpu as pltpu
from jax.sharding import PartitionSpec as P

MESH = pl.DeviceIdType.MESH
F32, BF16, I32 = jnp.float32, jnp.bfloat16, jnp.int32
D = 256
KEYS_DEV = 512
GROUPS_DEV = 32
ROWS = 4096
DELTA = 1024
CAP = 64
OWNERS = 32
VIEWS = 4
LANES = 128
PEERS = 64
HALF = 2048
OWNER_STEP = 11
PEER_STEP, PEER_STEP_INVERSE = 27, 19


def iota(shape, dim):
    return lax.broadcasted_iota(I32, shape, dim)


def dot(a, b):
    return jnp.dot(a, b, preferred_element_type=F32)


def one_hot(rows, height, base, values=None):
    at = iota((height, LANES), 0)
    parts = []
    for n, row in enumerate(rows):
        value = 1.0 if values is None else values[n]
        parts.append(jnp.where(at == row - base, value, 0.0).astype(BF16))
    return jnp.concatenate(parts, axis=1)


def places(table, key_ref, count):
    keys = [key_ref[s : s + 1, :] for s in range(DELTA // LANES)]
    at = iota((LANES, LANES), 0)
    hits = jnp.concatenate(
        [jnp.where(at == (k >> 7), 1.0, 0.0).astype(BF16) for k in keys], axis=1
    )
    found = dot(table, hits)
    slots, owners, lives, marks = [], [], [], []
    lane = iota((1, LANES), 1)
    owner_at = iota((OWNERS, LANES), 0)
    for s, k in enumerate(keys):
        cut = slice(s * LANES, (s + 1) * LANES)
        value = found[:LANES, cut] * 128.0 + found[LANES:, cut]
        slot = jnp.sum(jnp.where(at == (k & 127), value, 0.0), axis=0, keepdims=True).astype(I32)
        live = lane + s * LANES < count
        owner = jnp.where(live, slot >> 9, -1)
        slots.append(slot & (KEYS_DEV - 1))
        owners.append(owner)
        lives.append(live)
        marks.append(jnp.where(owner_at == owner, 1.0, 0.0))
    stacked = jnp.concatenate(marks, axis=0).astype(BF16)
    col = iota((LANES, 2 * LANES), 1)
    before = jnp.where((iota((LANES, 2 * LANES), 0) < col) | (col >= LANES), 1.0, 0.0).astype(BF16)
    counts = dot(stacked, before)
    carry = jnp.zeros((OWNERS, LANES), F32)
    spots = []
    for s in range(len(keys)):
        cut = slice(s * OWNERS, (s + 1) * OWNERS)
        rank = jnp.sum(marks[s] * (counts[cut, :LANES] + carry), axis=0, keepdims=True).astype(I32)
        spots.append(jnp.where(lives[s], owners[s] * CAP + rank, -1))
        carry = carry + counts[cut, LANES:]
    return slots, spots


def wait_bytes(ref, sem):
    pltpu.make_async_copy(ref, ref, sem).wait()


def kernel(
    key_slot, da_key, da_group, da_mult, da_count, db_key, db_mult, db_count, b_slot, b_weight,
    a_slot, a_weight, a_group, da_hbm, db_hbm, b_hbm, a_hbm,
    out,
    da_rows, db_rows, b_rows, a_rows, spot_ref, sign_ref, note_ref,
    db_send, da_send, db_info, da_info, db_recv, da_recv, db_info_recv, da_info_recv,
    part_b, quarter_b, got_b, full_b, part_db, quarter_db, got_db, full_db,
    pick, pick_d, table_a, table_w, terms, spots, near_send, near_recv, far_send, far_recv, own,
    load_sems, sems, near_sems,
):
    k, x = lax.axis_index("keys"), lax.axis_index("view")
    core = lax.rem(k, 2)
    partner = k + 1 - 2 * core
    seat = (k // 2) * VIEWS + x

    def load(src, dst, s):
        return pltpu.make_async_copy(src, dst, load_sems.at[s])

    loads = [
        load(db_hbm, db_rows, 0),
        load(da_hbm, da_rows, 1),
        load(b_hbm, b_rows, 2),
        load(a_hbm, a_rows, 3),
    ]
    for copy in loads:
        copy.start()

    def peer(j):
        t = lax.rem(seat + j, PEERS)
        return {"keys": (t // VIEWS) * 2 + core, "view": lax.rem(t, VIEWS)}

    def send(src, dst, sem_s, sem_r, device):
        return pltpu.make_async_remote_copy(
            src_ref=src, dst_ref=dst, send_sem=sem_s, recv_sem=sem_r, device_id=device,
            device_id_type=MESH,
        )

    barrier = pltpu.get_barrier_semaphore()

    def greet_same(j, carry):
        pl.semaphore_signal(barrier, inc=1, device_id=peer(j), device_id_type=MESH)
        return carry

    def greet_other(j, carry):
        to = {"keys": lax.rem(k + 2 * j + 1, OWNERS), "view": x}
        pl.semaphore_signal(barrier, inc=1, device_id=to, device_id_type=MESH)
        return carry

    with jax.named_scope("greet"):
        lax.fori_loop(1, PEERS, greet_same, 0)
        lax.fori_loop(0, OWNERS // 2, greet_other, 0)

    with jax.named_scope("lookup_b"):
        whole = key_slot[...]
        high = (whole >> 7).astype(F32).T
        low = (whole & 127).astype(F32).T
        table = jnp.concatenate([high, low], axis=0).astype(BF16)

        def look_up(r, key_ref, mult_ref, count_ref):
            slots, found = places(table, key_ref, count_ref[...])
            for s in range(8):
                cut = slice(s * LANES, (s + 1) * LANES)
                spot_ref[8 * r + s : 8 * r + s + 1, :] = found[s]
                sign_ref[8 * r + s : 8 * r + s + 1, :] = mult_ref[s : s + 1, :].astype(F32)
                group = da_group[s : s + 1, :]
                rows = [slots[s] >> 4, slots[s] & 15, group >> 6, group & 63]
                zero = jnp.zeros((4, LANES), F32)
                note_ref[r, :, cut] = jnp.concatenate(
                    [row.astype(F32) for row in rows] + [zero], axis=0
                ).astype(BF16)

        look_up(0, db_key, db_mult, db_count)

    def owner_of(i):
        return lax.rem(k + lax.rem(OWNER_STEP * i, OWNERS), OWNERS)

    def home(i):
        return lax.rem(OWNERS - lax.rem(OWNER_STEP * i, OWNERS), OWNERS)

    first = iota((8, LANES), 1) < CAP

    def packed(r, i, rows):
        at = iota((CAP, LANES), 0)
        picks = []
        for q in range(4):
            base = owner_of(4 * i + q) * CAP
            parts = []
            for s in range(8):
                spot = spot_ref[8 * r + s : 8 * r + s + 1, :]
                sign = sign_ref[8 * r + s : 8 * r + s + 1, :]
                parts.append(jnp.where(at == spot - base, sign, 0.0).astype(BF16))
            picks.append(jnp.concatenate(parts, axis=1))
        pick_rows = jnp.concatenate(picks, axis=0)
        blocks = dot(pick_rows, rows[...]).astype(BF16)
        note = jnp.abs(
            lax.dot_general(
                note_ref[r], pick_rows, (((1,), (1,)), ((), ())), preferred_element_type=F32
            )
        )
        info = jnp.concatenate(
            [
                note[0:1] * 16.0 + note[1:2],
                note[2:3] * 64.0 + note[3:4],
                jnp.zeros((6, 256), F32),
            ],
            axis=0,
        ).astype(I32)
        infos = []
        for q in range(4):
            v = info[:, (q // 2) * LANES : (q // 2 + 1) * LANES]
            turned = pltpu.roll(v, CAP, 1)
            infos.append(jnp.where(first, v, turned) if q % 2 == 0 else jnp.where(first, turned, v))
        return blocks, infos

    loads[0].wait()
    with jax.named_scope("barrier"):
        pl.semaphore_wait(barrier, PEERS - 1 + OWNERS // 2)

    def pack_b(i, carry):
        blocks, infos = packed(0, i, db_rows)
        for q in range(4):
            n = 4 * i + q
            db_info[n] = infos[q][0:1]
            for h in range(2):
                db_send[h, n] = blocks[q * CAP : (q + 1) * CAP, h * LANES : (h + 1) * LANES]
        for q in range(4):
            n = 4 * i + q

            @pl.when(n > 0)
            def _():
                to = {"keys": owner_of(n), "view": x}
                send(db_info.at[n], db_info_recv.at[home(n)], sems.at[0], sems.at[1], to).start()
                send(db_send.at[0, n], db_recv.at[0, home(n)], sems.at[2], sems.at[3], to).start()

        return carry

    with jax.named_scope("pack_b"):
        lax.fori_loop(0, 8, pack_b, 0)

    def second_half(n, carry):
        to = {"keys": owner_of(n), "view": x}
        send(db_send.at[1, n], db_recv.at[1, home(n)], sems.at[4], sems.at[5], to).start()
        return carry

    lax.fori_loop(1, OWNERS, second_half, 0)
    db_info_recv[0] = db_info[0]
    db_recv[0, 0] = db_send[0, 0]
    db_recv[1, 0] = db_send[1, 0]

    def quarter(at):
        return pl.ds(pl.multiple_of(at * 128, 128), 128)

    def across(part, got, s):
        for j in range(1, VIEWS):
            to = lax.rem(x + j, VIEWS)
            send(
                part.at[quarter(to)], got.at[j - 1], sems.at[s], sems.at[s + 1],
                {"keys": k, "view": to},
            ).start()

    def all_quarters(mine, full, s):
        for j in range(1, VIEWS):
            to = lax.rem(x + j, VIEWS)
            send(
                mine, full.at[quarter(x)], sems.at[s], sems.at[s + 1], {"keys": k, "view": to}
            ).start()

    loads[2].wait()
    with jax.named_scope("sum_b"):
        for m in range(2):
            acc = jnp.zeros((256, D), F32)
            for p in range(8):
                rows = [b_slot[4 * p + s : 4 * p + s + 1, :] for s in range(4)]
                values = [b_weight[4 * p + s : 4 * p + s + 1, :].astype(F32) for s in range(4)]
                hits = one_hot(rows, 256, 256 * m, values)
                acc = acc + dot(hits, b_rows[512 * p : 512 * (p + 1), :])
            part_b[256 * m : 256 * (m + 1), :] = acc
        across(part_b, got_b, 8)

    with jax.named_scope("lookup_a"):
        look_up(1, da_key, da_mult, da_count)
    loads[1].wait()

    def pack_a(i, carry):
        blocks, infos = packed(1, i, da_rows)
        for q in range(4):
            da_info[4 * i + q] = infos[q][0:2]
            da_send[4 * i + q] = blocks[q * CAP : (q + 1) * CAP, :]
        return carry

    with jax.named_scope("pack_a"):
        lax.fori_loop(0, 8, pack_a, 0)

    with jax.named_scope("wait_b"):
        wait_bytes(got_b, sems.at[9])
    quarter_b[...] = part_b[quarter(x), :] + got_b[0] + got_b[1] + got_b[2]
    all_quarters(quarter_b, full_b, 10)
    full_b[quarter(x), :] = quarter_b[...]

    left = iota((1, LANES), 1) < CAP

    def pair(ref, row, n):
        return jnp.where(left, ref[2 * n, row : row + 1, :], ref[2 * n + 1, row : row + 1, :])

    def sum_db(h):
        for m in range(2):
            acc = jnp.zeros((256, LANES), F32)
            for p in range(4):
                rows = [pair(db_info_recv, 0, 4 * p + s) for s in range(4)]
                blocks = db_recv[h, 8 * p : 8 * (p + 1)].reshape(512, LANES)
                acc = acc + dot(one_hot(rows, 256, 256 * m), blocks)
            part_db[h, 256 * m : 256 * (m + 1), :] = acc

    def finish_quarter(h):
        quarter_db[h] = part_db[h, quarter(x), :] + got_db[h, 0] + got_db[h, 1] + got_db[h, 2]
        all_quarters(quarter_db.at[h], full_db.at[h], 16 + 4 * h)
        full_db[h, quarter(x), :] = quarter_db[h]

    with jax.named_scope("wait_db0"):
        wait_bytes(db_info_recv.at[1:OWNERS], sems.at[1])
        wait_bytes(db_recv.at[0, 1:OWNERS], sems.at[3])
    sum_db(0)
    across(part_db.at[0], got_db.at[0], 14)

    at_lane = iota((LANES, LANES), 1)

    def pick_block(j, carry):
        row = a_slot[pl.ds(j, 1), :] + KEYS_DEV * a_weight[pl.ds(j, 1), :]
        cols = jnp.broadcast_to(row.astype(F32), (LANES, LANES)).T.astype(I32)
        slot, weight = cols & (KEYS_DEV - 1), (cols >> 9).astype(F32)
        at = pl.ds(pl.multiple_of(j * LANES, LANES), LANES)
        for q in range(4):
            pick[at, q * LANES : (q + 1) * LANES] = jnp.where(
                at_lane + q * LANES == slot, weight, 0.0
            ).astype(BF16)
        return carry

    with jax.named_scope("pick"):
        lax.fori_loop(0, 32, pick_block, 0)

    def place(group):
        device = group >> 5
        seat_g = (device >> 3) * VIEWS + (device & 3)
        other = ((device >> 2) & 1) ^ core
        turn = ((seat_g - seat) * PEER_STEP_INVERSE) & (PEERS - 1)
        return other * HALF + turn * GROUPS_DEV + (group & 31)

    spots[0:32, :] = place(a_group[...])

    with jax.named_scope("wait_rs0"):
        wait_bytes(got_db.at[0], sems.at[15])
    finish_quarter(0)

    with jax.named_scope("wait_db1"):
        wait_bytes(db_recv.at[1, 1:OWNERS], sems.at[5])
    sum_db(1)
    across(part_db.at[1], got_db.at[1], 18)

    def send_a(n, carry):
        to = {"keys": owner_of(n), "view": x}
        send(da_info.at[n], da_info_recv.at[home(n)], sems.at[6], sems.at[7], to).start()
        send(da_send.at[n], da_recv.at[home(n)], sems.at[12], sems.at[13], to).start()
        return carry

    lax.fori_loop(1, OWNERS, send_a, 0)
    da_info_recv[0] = da_info[0]
    da_recv[0] = da_send[0]

    def split(value):
        top = value.astype(BF16)
        return jnp.concatenate([top, (value - top.astype(F32)).astype(BF16)], axis=1)

    def a_terms(h):
        table_a[h] = split(full_db[h])

        def block(j, carry):
            at = pl.ds(pl.multiple_of(j * 1024, 1024), 1024)
            cut = slice(h * LANES, (h + 1) * LANES)
            both = dot(pick[at, :], table_a[h])
            value = (both[:, :LANES] + both[:, LANES:]) * a_rows[at, cut].astype(F32)
            terms[at, cut] = value.astype(BF16)
            return carry

        lax.fori_loop(0, 4, block, 0)

    loads[3].wait()
    with jax.named_scope("wait_ag0"):
        wait_bytes(full_db.at[0, 0:384], sems.at[17])
    with jax.named_scope("a_terms0"):
        a_terms(0)
    with jax.named_scope("wait_rs1"):
        wait_bytes(got_db.at[1], sems.at[19])
    finish_quarter(1)

    with jax.named_scope("wait_ag1"):
        wait_bytes(full_b.at[0:384], sems.at[11])
        wait_bytes(full_db.at[1, 0:384], sems.at[21])
    with jax.named_scope("a_terms1"):
        a_terms(1)

    for h in range(2):
        table_w[h] = split(full_db[h] + full_b[:, h * LANES : (h + 1) * LANES])

    with jax.named_scope("wait_da"):
        wait_bytes(da_info_recv.at[1:OWNERS], sems.at[7])
    with jax.named_scope("pick_d"):
        for n in range(16):
            spots[32 + n : 33 + n, :] = place(pair(da_info_recv, 1, n))
            cols = jnp.broadcast_to(
                pair(da_info_recv, 0, n).astype(F32), (LANES, LANES)
            ).T.astype(I32)
            for q in range(4):
                pick_d[n * LANES : (n + 1) * LANES, q * LANES : (q + 1) * LANES] = jnp.where(
                    at_lane + q * LANES == cols, 1.0, 0.0
                ).astype(BF16)
    with jax.named_scope("wait_da2"):
        wait_bytes(da_recv.at[1:OWNERS], sems.at[13])

    def d_block(j, carry):
        at = pl.ds(pl.multiple_of(j * 512, 512), 512)
        rows = da_recv[pl.ds(8 * j, 8)].reshape(512, D).astype(F32)
        for h in range(2):
            both = dot(pick_d[at, :], table_w[h])
            value = (both[:, :LANES] + both[:, LANES:]) * rows[:, h * LANES : (h + 1) * LANES]
            terms[
                pl.ds(pl.multiple_of(ROWS + j * 512, 512), 512), h * LANES : (h + 1) * LANES
            ] = value.astype(BF16)
        return carry

    with jax.named_scope("d_terms"):
        lax.fori_loop(0, 4, d_block, 0)

    def summed(base):
        acc = jnp.zeros((256, D), F32)
        for p in range(12):
            rows = [spots[4 * p + s : 4 * p + s + 1, :] for s in range(4)]
            acc = acc + dot(one_hot(rows, 256, base), terms[512 * p : 512 * (p + 1), :])
        return acc

    def to_partner(c):
        near_send[c] = summed(HALF + c * 256)
        send(
            near_send.at[c], near_recv.at[c], near_sems.at[0, c], near_sems.at[1, c],
            {"keys": partner, "view": x},
        ).start()

    def group_chunk(c, carry):
        @pl.when(c < 7)
        def _():
            to_partner(c + 1)

        acc = summed(c * 256)
        wait_bytes(near_recv.at[c], near_sems.at[1, c])
        acc = acc + near_recv[c]

        @pl.when(c == 0)
        def _():
            own[...] = acc[:GROUPS_DEV, :]

        far_send[pl.ds(8 * c, 8)] = acc.astype(BF16).reshape(8, GROUPS_DEV, D)

        def block(n, carry):
            j = lax.rem(PEER_STEP * n, PEERS)
            send(
                far_send.at[n], far_recv.at[PEERS - j], sems.at[22], sems.at[23], peer(j)
            ).start()
            return carry

        lax.fori_loop(lax.max(8 * c, 1), 8 * c + 8, block, 0)
        return carry

    with jax.named_scope("groups"):
        to_partner(0)
        lax.fori_loop(0, 8, group_chunk, 0)

    with jax.named_scope("wait_far"):
        wait_bytes(far_recv.at[1:PEERS], sems.at[23])
    with jax.named_scope("tail"):
        total = own[...]
        for j in range(1, PEERS):
            total = total + far_recv[j].astype(F32)
        out[...] = total

    wait_bytes(db_info.at[1:OWNERS], sems.at[0])
    wait_bytes(db_send.at[0, 1:OWNERS], sems.at[2])
    wait_bytes(db_send.at[1, 1:OWNERS], sems.at[4])
    wait_bytes(da_info.at[1:OWNERS], sems.at[6])
    wait_bytes(part_b.at[0:384], sems.at[8])
    wait_bytes(part_b.at[0:384], sems.at[10])
    wait_bytes(da_send.at[1:OWNERS], sems.at[12])
    for h in range(2):
        wait_bytes(part_db.at[h, 0:384], sems.at[14 + 4 * h])
        wait_bytes(part_db.at[h, 0:384], sems.at[16 + 4 * h])
    wait_bytes(far_send.at[1:PEERS], sems.at[22])
    for c in range(8):
        wait_bytes(near_send.at[c], near_sems.at[0, c])


def shards(
    key_slot, a_slot, a_group, a_weight, a_payload, b_slot, b_weight, b_payload, da_key, da_group,
    da_mult, da_payload, da_count, db_key, db_mult, db_payload, db_count,
):
    vmem = pl.BlockSpec(memory_space=pltpu.VMEM)
    hbm = pl.BlockSpec(memory_space=pl.ANY)

    def lanes(v):
        return v.reshape(-1, LANES)

    def one(v):
        return v.reshape(1, 1)

    def held(*shape, dtype=F32):
        return pltpu.VMEM(shape, dtype)

    return pl.pallas_call(
        kernel,
        out_shape=jax.ShapeDtypeStruct((GROUPS_DEV, D), F32),
        in_specs=[vmem] * 13 + [hbm] * 4,
        out_specs=vmem,
        scratch_shapes=[
            held(DELTA, D, dtype=BF16),
            held(DELTA, D, dtype=BF16),
            held(ROWS, D, dtype=BF16),
            held(ROWS, D, dtype=BF16),
            held(16, LANES, dtype=I32),
            held(16, LANES),
            held(2, 8, DELTA, dtype=BF16),
            held(2, OWNERS, CAP, LANES, dtype=BF16),
            held(OWNERS, CAP, D, dtype=BF16),
            held(OWNERS, 1, LANES, dtype=I32),
            held(OWNERS, 2, LANES, dtype=I32),
            held(2, OWNERS, CAP, LANES, dtype=BF16),
            held(OWNERS, CAP, D, dtype=BF16),
            held(OWNERS, 1, LANES, dtype=I32),
            held(OWNERS, 2, LANES, dtype=I32),
            held(KEYS_DEV, D),
            held(128, D),
            held(3, 128, D),
            held(KEYS_DEV, D),
            held(2, KEYS_DEV, LANES),
            held(2, 128, LANES),
            held(2, 3, 128, LANES),
            held(2, KEYS_DEV, LANES),
            held(ROWS, KEYS_DEV, dtype=BF16),
            held(OWNERS * CAP, KEYS_DEV, dtype=BF16),
            held(2, KEYS_DEV, D, dtype=BF16),
            held(2, KEYS_DEV, D, dtype=BF16),
            held(ROWS + OWNERS * CAP, D, dtype=BF16),
            held(48, LANES, dtype=I32),
            held(8, 256, D),
            held(8, 256, D),
            held(PEERS, GROUPS_DEV, D, dtype=BF16),
            held(PEERS, GROUPS_DEV, D, dtype=BF16),
            held(GROUPS_DEV, D),
            pltpu.SemaphoreType.DMA((4,)),
            pltpu.SemaphoreType.DMA((24,)),
            pltpu.SemaphoreType.DMA((2, 8)),
        ],
        compiler_params=pltpu.CompilerParams(
            collective_id=0, has_side_effects=True, vmem_limit_bytes=56 * 1024 * 1024
        ),
    )(
        lanes(key_slot), lanes(da_key), lanes(da_group), lanes(da_mult), one(da_count),
        lanes(db_key), lanes(db_mult), one(db_count), lanes(b_slot), lanes(b_weight),
        lanes(a_slot), lanes(a_weight), lanes(a_group), da_payload, db_payload, b_payload,
        a_payload,
    )


def solution(mesh):
    rows = P(("keys", "view"))
    wide = P(("keys", "view"), None)
    placed = (
        P(), rows, rows, rows, wide, rows, rows, wide, rows, rows, rows, wide, rows, rows, rows,
        wide, rows,
    )
    return jax.shard_map(
        shards, mesh=mesh, in_specs=placed, out_specs=wide, check_vma=False
    )
```

```python
import jax
import jax.numpy as jnp
from jax import lax
from jax.experimental import pallas as pl
from jax.experimental.pallas import tpu as pltpu
from jax.sharding import PartitionSpec as P

MESH = pl.DeviceIdType.MESH
F32, BF16, I32 = jnp.float32, jnp.bfloat16, jnp.int32
D = 256
KEYS_DEV = 512
GROUPS_DEV = 32
ROWS = 4096
DELTA = 1024
CAP = 64
OWNERS = 32
VIEWS = 4
LANES = 128
PEERS = 64
HALF = 2048
OWNER_STEP = 11
CHUNK = 512


def apart(code):
    return sum((0, 1, 2, 1)[d] for d in (code >> 4, (code >> 2) & 3, code & 3))


FAR_FIRST = sorted(range(PEERS), key=lambda code: (-apart(code), (code * 27) % PEERS))
RANK = [FAR_FIRST.index(code) for code in range(PEERS)]


def iota(shape, dim):
    return lax.broadcasted_iota(I32, shape, dim)


def dot(a, b):
    return jnp.dot(a, b, preferred_element_type=F32)


def one_hot(rows, height, base, values=None):
    at = iota((height, LANES), 0)
    parts = []
    for n, row in enumerate(rows):
        value = 1.0 if values is None else values[n]
        parts.append(jnp.where(at == row - base, value, 0.0).astype(BF16))
    return jnp.concatenate(parts, axis=1)


def places(table, key_ref, count):
    keys = [key_ref[s : s + 1, :] for s in range(DELTA // LANES)]
    at = iota((LANES, LANES), 0)
    hits = jnp.concatenate(
        [jnp.where(at == (k >> 7), 1.0, 0.0).astype(BF16) for k in keys], axis=1
    )
    found = dot(table, hits)
    slots, owners, lives, marks = [], [], [], []
    lane = iota((1, LANES), 1)
    owner_at = iota((OWNERS, LANES), 0)
    for s, k in enumerate(keys):
        cut = slice(s * LANES, (s + 1) * LANES)
        value = found[:LANES, cut] * 128.0 + found[LANES:, cut]
        slot = jnp.sum(jnp.where(at == (k & 127), value, 0.0), axis=0, keepdims=True).astype(I32)
        live = lane + s * LANES < count
        owner = jnp.where(live, slot >> 9, -1)
        slots.append(slot & (KEYS_DEV - 1))
        owners.append(owner)
        lives.append(live)
        marks.append(jnp.where(owner_at == owner, 1.0, 0.0))
    stacked = jnp.concatenate(marks, axis=0).astype(BF16)
    col = iota((LANES, 2 * LANES), 1)
    before = jnp.where((iota((LANES, 2 * LANES), 0) < col) | (col >= LANES), 1.0, 0.0).astype(BF16)
    counts = dot(stacked, before)
    carry = jnp.zeros((OWNERS, LANES), F32)
    spots, ranks = [], []
    for s in range(len(keys)):
        cut = slice(s * OWNERS, (s + 1) * OWNERS)
        rank = jnp.sum(marks[s] * (counts[cut, :LANES] + carry), axis=0, keepdims=True).astype(I32)
        ranks.append(rank)
        spots.append(jnp.where(lives[s], owners[s] * CAP + rank, -1))
        carry = carry + counts[cut, LANES:]
    return slots, spots, marks, ranks


def by_place(marks, ranks, values):
    rank_at = iota((LANES, LANES), 0) & (CAP - 1)
    there = jnp.concatenate(
        [jnp.where(rank_at == rank, 1.0, 0.0).astype(BF16) for rank in ranks], axis=1
    )
    rows = jnp.concatenate(
        [
            jnp.concatenate([mark * v.astype(F32) for mark, v in zip(marks, value)], axis=1)
            for value in values
        ],
        axis=0,
    ).astype(BF16)
    return lax.dot_general(rows, there, (((1,), (1,)), ((), ())), preferred_element_type=F32)


def wait_bytes(ref, sem):
    pltpu.make_async_copy(ref, ref, sem).wait()


def kernel(
    key_slot, da_key, da_group, da_mult, db_key, db_mult, b_slot, b_weight, a_slot, a_weight,
    a_group, da_count_hbm, db_count_hbm, da_hbm, db_hbm, b_hbm, a_hbm,
    out,
    da_count, db_count, da_rows, db_rows, b_rows, a_rows, spot_ref, sign_ref,
    db_send, da_send, db_info, da_info, db_recv, da_recv, db_info_recv, da_info_recv,
    part_b, quarter_b, got_b, full_b, part_db, quarter_db, got_db, full_db,
    pick, pick_d, table_a, table_w, terms, spots, near_send, near_recv, far_send, far_recv, own, total_ref,
    load_sems, sems, near_sems, planes,
):
    k, x = lax.axis_index("keys"), lax.axis_index("view")
    core = lax.rem(k, 2)
    partner = k + 1 - 2 * core
    y, z = k // 8, lax.rem(k // 2, 4)

    def load(src, dst, s):
        return pltpu.make_async_copy(src, dst, load_sems.at[s])

    loads = [
        load(db_hbm, db_rows, 0),
        load(da_hbm, da_rows, 1),
        load(b_hbm, b_rows, 2),
        load(a_hbm, a_rows, 3),
        load(da_count_hbm, da_count, 4),
        load(db_count_hbm, db_count, 5),
    ]
    loads[5].start()
    loads[0].start()

    def peer(code):
        to_y, to_z = lax.rem(y + (code >> 4), 4), lax.rem(z + ((code >> 2) & 3), 4)
        return {"keys": (to_y * 4 + to_z) * 2 + core, "view": lax.rem(x + (code & 3), VIEWS)}

    def send(src, dst, sem_s, sem_r, device):
        return pltpu.make_async_remote_copy(
            src_ref=src, dst_ref=dst, send_sem=sem_s, recv_sem=sem_r, device_id=device,
            device_id_type=MESH,
        )

    barrier = pltpu.get_barrier_semaphore()

    def greet(j, carry):
        to = {"keys": lax.rem(k + j, OWNERS), "view": x}
        pl.semaphore_signal(barrier, inc=1, device_id=to, device_id_type=MESH)
        return carry

    with jax.named_scope("greet"):
        lax.fori_loop(1, OWNERS, greet, 0)
        for j in range(1, VIEWS):
            to = {"keys": k, "view": lax.rem(x + j, VIEWS)}
            pl.semaphore_signal(barrier, inc=1, device_id=to, device_id_type=MESH)
        for n in (4, 1, 2, 3):
            loads[n].start()

    with jax.named_scope("lookup_b"):
        whole = key_slot[...]
        high = (whole >> 7).astype(F32).T
        low = (whole & 127).astype(F32).T
        table = jnp.concatenate([high, low], axis=0).astype(BF16)

        def look_up(r, key_ref, mult_ref, count_ref):
            slots, found, marks, ranks = places(table, key_ref, count_ref[0])
            for s in range(8):
                spot_ref[8 * r + s : 8 * r + s + 1, :] = found[s]
                sign_ref[8 * r + s : 8 * r + s + 1, :] = mult_ref[s : s + 1, :].astype(F32)
            return slots, marks, ranks

        loads[5].wait()
        slots_b, marks_b, ranks_b = look_up(0, db_key, db_mult, db_count)
        note = by_place(
            marks_b, ranks_b, [[v >> 4 for v in slots_b], [v & 15 for v in slots_b]]
        )
        note = (note[:OWNERS] * 16.0 + note[OWNERS:]).astype(I32)
        for n in range(OWNERS):
            db_info[n] = note[n : n + 1, :]

    def home(i):
        return lax.rem(OWNER_STEP * i, OWNERS)

    def owner_of(i):
        code = home(i)
        to_y, to_z = lax.rem(y + code // 8, 4), lax.rem(z + lax.rem(code // 2, 4), 4)
        return (to_y * 4 + to_z) * 2 + lax.rem(core + lax.rem(code, 2), 2)

    def packed(r, i, rows):
        at = iota((CAP, LANES), 0)
        picks = []
        for q in range(8):
            base = owner_of(8 * i + q) * CAP
            parts = []
            for s in range(8):
                spot = spot_ref[8 * r + s : 8 * r + s + 1, :]
                sign = sign_ref[8 * r + s : 8 * r + s + 1, :]
                parts.append(jnp.where(at == spot - base, sign, 0.0).astype(BF16))
            picks.append(jnp.concatenate(parts, axis=1))
        return dot(jnp.concatenate(picks, axis=0), rows[...]).astype(BF16)

    loads[0].wait()

    def pack_b(i, carry):
        blocks = packed(0, i, db_rows)
        for q in range(8):
            n = 8 * i + q
            for h in range(2):
                db_send[h, n] = blocks[q * CAP : (q + 1) * CAP, h * LANES : (h + 1) * LANES]
        return carry

    with jax.named_scope("pack_b"):
        lax.fori_loop(0, 4, pack_b, 0)

    with jax.named_scope("barrier"):
        pl.semaphore_wait(barrier, OWNERS - 1 + VIEWS - 1)

    def first_half(n, carry):
        to = {"keys": owner_of(n), "view": x}
        send(db_info.at[owner_of(n)], db_info_recv.at[home(n)], sems.at[0], sems.at[1], to).start()
        send(db_send.at[0, n], db_recv.at[0, home(n)], sems.at[2], sems.at[3], to).start()
        return carry

    def second_half(n, carry):
        to = {"keys": owner_of(n), "view": x}
        send(db_send.at[1, n], db_recv.at[1, home(n)], sems.at[4], sems.at[5], to).start()
        return carry

    with jax.named_scope("send_b"):
        lax.fori_loop(1, OWNERS, first_half, 0)
        for j in range(1, VIEWS):
            to = {"keys": k, "view": lax.rem(x + j, VIEWS)}
            pl.semaphore_signal(planes, inc=1, device_id=to, device_id_type=MESH)
        lax.fori_loop(1, OWNERS, second_half, 0)
    db_info_recv[0] = db_info[k]
    db_recv[0, 0] = db_send[0, 0]
    db_recv[1, 0] = db_send[1, 0]

    def quarter(at):
        return pl.ds(pl.multiple_of(at * 128, 128), 128)

    def across(part, got, s):
        for j in range(1, VIEWS):
            to = lax.rem(x + j, VIEWS)
            send(
                part.at[quarter(to)], got.at[j - 1], sems.at[s], sems.at[s + 1],
                {"keys": k, "view": to},
            ).start()

    def all_quarters(mine, full, s):
        for j in range(1, VIEWS):
            to = lax.rem(x + j, VIEWS)
            send(
                mine, full.at[quarter(x)], sems.at[s], sems.at[s + 1], {"keys": k, "view": to}
            ).start()

    loads[2].wait()
    with jax.named_scope("sum_b"):
        for m in range(2):
            acc = jnp.zeros((256, D), F32)
            for p in range(8):
                rows = [b_slot[4 * p + s : 4 * p + s + 1, :] for s in range(4)]
                values = [b_weight[4 * p + s : 4 * p + s + 1, :].astype(F32) for s in range(4)]
                hits = one_hot(rows, 256, 256 * m, values)
                acc = acc + dot(hits, b_rows[512 * p : 512 * (p + 1), :])
            part_b[256 * m : 256 * (m + 1), :] = acc
        across(part_b, got_b, 8)

    with jax.named_scope("lookup_a"):
        loads[4].wait()
        slots_a, marks_a, ranks_a = look_up(1, da_key, da_mult, da_count)
        groups = [da_group[s : s + 1, :] for s in range(8)]
        note = by_place(
            marks_a,
            ranks_a,
            [
                [v >> 4 for v in slots_a],
                [v & 15 for v in slots_a],
                [v >> 6 for v in groups],
                [v & 63 for v in groups],
            ],
        )
        slot_note = (note[:OWNERS] * 16.0 + note[OWNERS : 2 * OWNERS]).astype(I32)
        group_note = (note[2 * OWNERS : 3 * OWNERS] * 64.0 + note[3 * OWNERS :]).astype(I32)
        for n in range(OWNERS):
            da_info[n] = jnp.concatenate([slot_note[n : n + 1, :], group_note[n : n + 1, :]], axis=0)
    loads[1].wait()

    def pack_a(i, carry):
        blocks = packed(1, i, da_rows)
        for q in range(8):
            da_send[8 * i + q] = blocks[q * CAP : (q + 1) * CAP, :]
        return carry

    with jax.named_scope("pack_a"):
        lax.fori_loop(0, 4, pack_a, 0)

    def send_a_info(n, carry):
        to = {"keys": owner_of(n), "view": x}
        send(da_info.at[owner_of(n)], da_info_recv.at[home(n)], sems.at[6], sems.at[7], to).start()
        return carry

    lax.fori_loop(1, OWNERS, send_a_info, 0)
    da_info_recv[0] = da_info[k]
    da_recv[0] = da_send[0]

    left = iota((1, LANES), 1) < CAP

    def pair(ref, row, n):
        return jnp.where(left, ref[2 * n, row : row + 1, :], ref[2 * n + 1, row : row + 1, :])

    def sum_db(h):
        for m in range(2):
            acc = jnp.zeros((256, LANES), F32)
            for p in range(4):
                rows = [pair(db_info_recv, 0, 4 * p + s) for s in range(4)]
                blocks = db_recv[h, 8 * p : 8 * (p + 1)].reshape(512, LANES)
                acc = acc + dot(one_hot(rows, 256, 256 * m), blocks)
            part_db[h, 256 * m : 256 * (m + 1), :] = acc

    def finish_quarter(h):
        quarter_db[h] = part_db[h, quarter(x), :] + got_db[h, 0] + got_db[h, 1] + got_db[h, 2]
        all_quarters(quarter_db.at[h], full_db.at[h], 16 + 4 * h)
        full_db[h, quarter(x), :] = quarter_db[h]

    with jax.named_scope("wait_db0"):
        wait_bytes(db_info_recv.at[1:OWNERS], sems.at[1])
        wait_bytes(db_recv.at[0, 1:OWNERS], sems.at[3])
    sum_db(0)
    across(part_db.at[0], got_db.at[0], 14)

    with jax.named_scope("wait_b"):
        wait_bytes(got_b, sems.at[9])
    whole_b = part_b[quarter(x), :] + got_b[0] + got_b[1] + got_b[2]
    for h in range(2):
        quarter_b[h] = whole_b[:, h * LANES : (h + 1) * LANES]
        full_b[h, quarter(x), :] = quarter_b[h]
    all_quarters(quarter_b.at[0], full_b.at[0], 10)

    at_lane = iota((LANES, LANES), 1)

    def pick_block(j, carry):
        row = a_slot[pl.ds(j, 1), :] + KEYS_DEV * a_weight[pl.ds(j, 1), :]
        cols = jnp.broadcast_to(row.astype(F32), (LANES, LANES)).T.astype(I32)
        slot, weight = cols & (KEYS_DEV - 1), (cols >> 9).astype(F32)
        at = pl.ds(pl.multiple_of(j * LANES, LANES), LANES)
        for q in range(4):
            pick[at, q * LANES : (q + 1) * LANES] = jnp.where(
                at_lane + q * LANES == slot, weight, 0.0
            ).astype(BF16)
        return carry

    with jax.named_scope("pick"):
        lax.fori_loop(0, 32, pick_block, 0)

    def place(group):
        to_y, to_z, to_x = group >> 10, (group >> 8) & 3, (group >> 5) & 3
        code = ((to_y - y) & 3) * 16 + ((to_z - z) & 3) * 4 + ((to_x - x) & 3)
        rank = jnp.zeros_like(code)
        for n in range(PEERS):
            rank = jnp.where(code == n, RANK[n], rank)
        other = ((group >> 7) & 1) ^ core
        return other * HALF + rank * GROUPS_DEV + (group & 31)

    spots[0:32, :] = place(a_group[...])

    with jax.named_scope("wait_rs0"):
        wait_bytes(got_db.at[0], sems.at[15])
    finish_quarter(0)

    with jax.named_scope("wait_db1"):
        wait_bytes(db_recv.at[1, 1:OWNERS], sems.at[5])
    sum_db(1)
    across(part_db.at[1], got_db.at[1], 18)

    def send_a(n, carry):
        to = {"keys": owner_of(n), "view": x}
        send(da_send.at[n], da_recv.at[home(n)], sems.at[12], sems.at[13], to).start()
        return carry

    lax.fori_loop(1, OWNERS, send_a, 0)

    with jax.named_scope("wait_da_info"):
        wait_bytes(da_info_recv.at[1:OWNERS], sems.at[7])
    with jax.named_scope("pick_d"):
        groups_d = jnp.concatenate([pair(da_info_recv, 1, n) for n in range(16)], axis=0)
        spots[32:48, :] = place(groups_d)
        for n in range(16):
            cols = jnp.broadcast_to(
                pair(da_info_recv, 0, n).astype(F32), (LANES, LANES)
            ).T.astype(I32)
            for q in range(4):
                pick_d[n * LANES : (n + 1) * LANES, q * LANES : (q + 1) * LANES] = jnp.where(
                    at_lane + q * LANES == cols, 1.0, 0.0
                ).astype(BF16)

    def split(value):
        top = value.astype(BF16)
        return jnp.concatenate([top, (value - top.astype(F32)).astype(BF16)], axis=1)

    def a_terms(h):
        table_a[h] = split(full_db[h])

        def block(j, carry):
            at = pl.ds(pl.multiple_of(j * 1024, 1024), 1024)
            cut = slice(h * LANES, (h + 1) * LANES)
            both = dot(pick[at, :], table_a[h])
            value = (both[:, :LANES] + both[:, LANES:]) * a_rows[at, cut].astype(F32)
            terms[at, cut] = value.astype(BF16)
            return carry

        lax.fori_loop(0, 4, block, 0)

    with jax.named_scope("wait_rs1"):
        wait_bytes(got_db.at[1], sems.at[19])
    finish_quarter(1)
    all_quarters(quarter_b.at[1], full_b.at[1], 24)

    loads[3].wait()
    with jax.named_scope("wait_ag0"):
        wait_bytes(full_db.at[0, 0:384], sems.at[17])
    with jax.named_scope("a_terms0"):
        a_terms(0)

    with jax.named_scope("wait_ag1"):
        wait_bytes(full_db.at[1, 0:384], sems.at[21])
    with jax.named_scope("a_terms1"):
        a_terms(1)

    with jax.named_scope("wait_ag_b"):
        wait_bytes(full_b.at[0, 0:384], sems.at[11])
        wait_bytes(full_b.at[1, 0:384], sems.at[25])
    for h in range(2):
        table_w[h] = split(full_db[h] + full_b[h])

    with jax.named_scope("wait_da"):
        wait_bytes(da_recv.at[1:OWNERS], sems.at[13])

    def d_block(j, carry):
        at = pl.ds(pl.multiple_of(j * 512, 512), 512)
        rows = da_recv[pl.ds(8 * j, 8)].reshape(512, D).astype(F32)
        for h in range(2):
            both = dot(pick_d[at, :], table_w[h])
            value = (both[:, :LANES] + both[:, LANES:]) * rows[:, h * LANES : (h + 1) * LANES]
            terms[
                pl.ds(pl.multiple_of(ROWS + j * 512, 512), 512), h * LANES : (h + 1) * LANES
            ] = value.astype(BF16)
        return carry

    with jax.named_scope("d_terms"):
        lax.fori_loop(0, 4, d_block, 0)

    def summed(base):
        acc = jnp.zeros((CHUNK, D), F32)
        for p in range(12):
            rows = [spots[4 * p + s : 4 * p + s + 1, :] for s in range(4)]
            acc = acc + dot(one_hot(rows, CHUNK, base), terms[512 * p : 512 * (p + 1), :])
        return acc

    chunks = HALF // CHUNK
    blocks_each = CHUNK // GROUPS_DEV
    steps = [(other, c) for c in range(chunks) for other in (1, 0)]

    def group_step(t, carry):
        base = 0
        for n, (other, c) in enumerate(steps):
            base = jnp.where(t == n, other * HALF + c * CHUNK, base)
        total_ref[...] = summed(base)
        for n, (other, c) in enumerate(steps):

            @pl.when(t == n)
            def _(other=other, c=c):
                if other:
                    near_send[c] = total_ref[...]
                    send(
                        near_send.at[c], near_recv.at[c], near_sems.at[0, c], near_sems.at[1, c],
                        {"keys": partner, "view": x},
                    ).start()
                    return
                wait_bytes(near_recv.at[c], near_sems.at[1, c])
                acc = total_ref[...] + near_recv[c]
                if c + 1 == chunks:
                    own[...] = acc[CHUNK - GROUPS_DEV :, :]
                far_send[c * blocks_each : (c + 1) * blocks_each] = acc.astype(BF16).reshape(
                    blocks_each, GROUPS_DEV, D
                )
                if c == 0:
                    pl.semaphore_wait(planes, VIEWS - 1)
                for m in range(c * blocks_each, (c + 1) * blocks_each):
                    code = FAR_FIRST[m]
                    if code:
                        send(
                            far_send.at[m], far_recv.at[code], sems.at[22], sems.at[23], peer(code)
                        ).start()

        return carry

    with jax.named_scope("groups"):
        lax.fori_loop(0, len(steps), group_step, 0)

    with jax.named_scope("wait_far"):
        wait_bytes(far_recv.at[1:PEERS], sems.at[23])
    with jax.named_scope("tail"):
        total = own[...]
        for j in range(1, PEERS):
            total = total + far_recv[j].astype(F32)
        out[...] = total

    wait_bytes(db_info.at[1:OWNERS], sems.at[0])
    wait_bytes(db_send.at[0, 1:OWNERS], sems.at[2])
    wait_bytes(db_send.at[1, 1:OWNERS], sems.at[4])
    wait_bytes(da_info.at[1:OWNERS], sems.at[6])
    wait_bytes(part_b.at[0:384], sems.at[8])
    wait_bytes(full_b.at[0, 0:384], sems.at[10])
    wait_bytes(full_b.at[1, 0:384], sems.at[24])
    wait_bytes(da_send.at[1:OWNERS], sems.at[12])
    for h in range(2):
        wait_bytes(part_db.at[h, 0:384], sems.at[14 + 4 * h])
        wait_bytes(part_db.at[h, 0:384], sems.at[16 + 4 * h])
    wait_bytes(far_send.at[0 : PEERS - 1], sems.at[22])
    for c in range(chunks):
        wait_bytes(near_send.at[c], near_sems.at[0, c])


def shards(
    key_slot, a_slot, a_group, a_weight, a_payload, b_slot, b_weight, b_payload, da_key, da_group,
    da_mult, da_payload, da_count, db_key, db_mult, db_payload, db_count,
):
    vmem = pl.BlockSpec(memory_space=pltpu.VMEM)
    hbm = pl.BlockSpec(memory_space=pl.ANY)
    fixed = pl.BlockSpec(memory_space=pltpu.HBM)

    def lanes(v):
        return v.reshape(-1, LANES)

    def held(*shape, dtype=F32):
        return pltpu.VMEM(shape, dtype)

    return pl.pallas_call(
        kernel,
        out_shape=jax.ShapeDtypeStruct((GROUPS_DEV, D), F32),
        in_specs=[vmem] * 11 + [fixed] * 2 + [hbm] * 4,
        out_specs=vmem,
        scratch_shapes=[
            pltpu.SMEM((1,), I32),
            pltpu.SMEM((1,), I32),
            held(DELTA, D, dtype=BF16),
            held(DELTA, D, dtype=BF16),
            held(ROWS, D, dtype=BF16),
            held(ROWS, D, dtype=BF16),
            held(16, LANES, dtype=I32),
            held(16, LANES),
            held(2, OWNERS, CAP, LANES, dtype=BF16),
            held(OWNERS, CAP, D, dtype=BF16),
            held(OWNERS, 1, LANES, dtype=I32),
            held(OWNERS, 2, LANES, dtype=I32),
            held(2, OWNERS, CAP, LANES, dtype=BF16),
            held(OWNERS, CAP, D, dtype=BF16),
            held(OWNERS, 1, LANES, dtype=I32),
            held(OWNERS, 2, LANES, dtype=I32),
            held(KEYS_DEV, D),
            held(2, 128, LANES),
            held(3, 128, D),
            held(2, KEYS_DEV, LANES),
            held(2, KEYS_DEV, LANES),
            held(2, 128, LANES),
            held(2, 3, 128, LANES),
            held(2, KEYS_DEV, LANES),
            held(ROWS, KEYS_DEV, dtype=BF16),
            held(OWNERS * CAP, KEYS_DEV, dtype=BF16),
            held(2, KEYS_DEV, D, dtype=BF16),
            held(2, KEYS_DEV, D, dtype=BF16),
            held(ROWS + OWNERS * CAP, D, dtype=BF16),
            held(48, LANES, dtype=I32),
            held(HALF // CHUNK, CHUNK, D),
            held(HALF // CHUNK, CHUNK, D),
            held(PEERS, GROUPS_DEV, D, dtype=BF16),
            held(PEERS, GROUPS_DEV, D, dtype=BF16),
            held(GROUPS_DEV, D),
            held(CHUNK, D),
            pltpu.SemaphoreType.DMA((6,)),
            pltpu.SemaphoreType.DMA((26,)),
            pltpu.SemaphoreType.DMA((2, HALF // CHUNK)),
            pltpu.SemaphoreType.REGULAR,
        ],
        compiler_params=pltpu.CompilerParams(
            collective_id=0, has_side_effects=True, vmem_limit_bytes=56 * 1024 * 1024
        ),
    )(
        lanes(key_slot), lanes(da_key), lanes(da_group), lanes(da_mult), lanes(db_key),
        lanes(db_mult), lanes(b_slot), lanes(b_weight), lanes(a_slot), lanes(a_weight),
        lanes(a_group), da_count, db_count, da_payload, db_payload, b_payload, a_payload,
    )


def solution(mesh):
    rows = P(("keys", "view"))
    wide = P(("keys", "view"), None)
    placed = (
        P(), rows, rows, rows, wide, rows, rows, wide, rows, rows, rows, wide, rows, rows, rows,
        wide, rows,
    )
    return jax.shard_map(
        shards, mesh=mesh, in_specs=placed, out_specs=wide, check_vma=False
    )
```

```python
import jax
import jax.numpy as jnp
from jax import lax
from jax.experimental import pallas as pl
from jax.experimental.pallas import tpu as pltpu
from jax.sharding import PartitionSpec as P

MESH = pl.DeviceIdType.MESH
F32, BF16, I32 = jnp.float32, jnp.bfloat16, jnp.int32
D = 256
KEYS_DEV = 512
GROUPS_DEV = 32
ROWS = 4096
DELTA = 1024
CAP = 64
OWNERS = 32
VIEWS = 4
LANES = 128
PEERS = 64
HALF = 2048
OWNER_STEP = 11
CHUNK, SMALL = 512, 256
CHUNKS = [(0, 256), (256, 512), (768, 512), (1280, 512), (1792, 256)]
EARLY = 3


def apart(code):
    return sum((0, 1, 2, 1)[d] for d in (code >> 4, (code >> 2) & 3, code & 3))


FAR_FIRST = sorted(range(PEERS), key=lambda code: (-apart(code), (code * 27) % PEERS))
RANK = [FAR_FIRST.index(code) for code in range(PEERS)]


def iota(shape, dim):
    return lax.broadcasted_iota(I32, shape, dim)


def dot(a, b):
    return jnp.dot(a, b, preferred_element_type=F32)


def one_hot(rows, height, base, values=None):
    at = iota((height, LANES), 0)
    parts = []
    for n, row in enumerate(rows):
        value = 1.0 if values is None else values[n]
        parts.append(jnp.where(at == row - base, value, 0.0).astype(BF16))
    return jnp.concatenate(parts, axis=1)


def places(table, key_ref, count):
    keys = [key_ref[s : s + 1, :] for s in range(DELTA // LANES)]
    at = iota((LANES, LANES), 0)
    hits = jnp.concatenate(
        [jnp.where(at == (k >> 7), 1.0, 0.0).astype(BF16) for k in keys], axis=1
    )
    found = dot(table, hits)
    slots, owners, lives, marks = [], [], [], []
    lane = iota((1, LANES), 1)
    owner_at = iota((OWNERS, LANES), 0)
    for s, k in enumerate(keys):
        cut = slice(s * LANES, (s + 1) * LANES)
        value = found[:LANES, cut] * 128.0 + found[LANES:, cut]
        slot = jnp.sum(jnp.where(at == (k & 127), value, 0.0), axis=0, keepdims=True).astype(I32)
        live = lane + s * LANES < count
        owner = jnp.where(live, slot >> 9, -1)
        slots.append(slot & (KEYS_DEV - 1))
        owners.append(owner)
        lives.append(live)
        marks.append(jnp.where(owner_at == owner, 1.0, 0.0))
    stacked = jnp.concatenate(marks, axis=0).astype(BF16)
    col = iota((LANES, 2 * LANES), 1)
    before = jnp.where((iota((LANES, 2 * LANES), 0) < col) | (col >= LANES), 1.0, 0.0).astype(BF16)
    counts = dot(stacked, before)
    carry = jnp.zeros((OWNERS, LANES), F32)
    spots, ranks = [], []
    for s in range(len(keys)):
        cut = slice(s * OWNERS, (s + 1) * OWNERS)
        rank = jnp.sum(marks[s] * (counts[cut, :LANES] + carry), axis=0, keepdims=True).astype(I32)
        ranks.append(rank)
        spots.append(jnp.where(lives[s], owners[s] * CAP + rank, -1))
        carry = carry + counts[cut, LANES:]
    return slots, spots, marks, ranks


def by_place(marks, ranks, values):
    rank_at = iota((LANES, LANES), 0) & (CAP - 1)
    there = jnp.concatenate(
        [jnp.where(rank_at == rank, 1.0, 0.0).astype(BF16) for rank in ranks], axis=1
    )
    rows = jnp.concatenate(
        [
            jnp.concatenate([mark * v.astype(F32) for mark, v in zip(marks, value)], axis=1)
            for value in values
        ],
        axis=0,
    ).astype(BF16)
    return lax.dot_general(rows, there, (((1,), (1,)), ((), ())), preferred_element_type=F32)


def wait_bytes(ref, sem):
    pltpu.make_async_copy(ref, ref, sem).wait()


def kernel(
    key_slot_hbm, db_key_hbm, db_mult_hbm, db_count_hbm, db_hbm, b_slot_hbm, b_weight_hbm, b_hbm,
    da_key_hbm, da_group_hbm, da_mult_hbm, da_count_hbm, da_hbm, a_slot_hbm, a_weight_hbm,
    a_group_hbm, a_hbm,
    out,
    key_slot, db_key, db_mult, b_slot, b_weight, da_key, da_group, da_mult, a_slot, a_weight,
    a_group, da_count, db_count, da_rows, db_rows, b_rows, a_rows, spot_ref, sign_ref,
    db_send, da_send, db_info, da_info, db_recv, da_recv, db_info_recv, da_info_recv,
    part_b, quarter_b, got_b, full_b, part_db, quarter_db, got_db, full_db,
    pick, pick_d, table_a, table_w, terms, spots, near_send, near_recv, far_send, far_recv, own, big_sum, small_sum, early,
    load_sems, sems, near_sems, part_sems, planes,
):
    k, x = lax.axis_index("keys"), lax.axis_index("view")
    core = lax.rem(k, 2)
    partner = k + 1 - 2 * core
    y, z = k // 8, lax.rem(k // 2, 4)

    pairs = (
        (key_slot_hbm, key_slot), (db_key_hbm, db_key), (db_mult_hbm, db_mult),
        (db_count_hbm, db_count), (db_hbm, db_rows), (b_slot_hbm, b_slot),
        (b_weight_hbm, b_weight), (b_hbm, b_rows), (da_key_hbm, da_key),
        (da_group_hbm, da_group), (da_mult_hbm, da_mult), (da_count_hbm, da_count),
        (da_hbm, da_rows), (a_slot_hbm, a_slot), (a_weight_hbm, a_weight),
        (a_group_hbm, a_group), (a_hbm, a_rows),
    )
    loads = [
        pltpu.make_async_copy(src, dst, load_sems.at[n]) for n, (src, dst) in enumerate(pairs)
    ]
    for n in range(4):
        loads[n].start()

    def peer(code):
        to_y, to_z = lax.rem(y + (code >> 4), 4), lax.rem(z + ((code >> 2) & 3), 4)
        return {"keys": (to_y * 4 + to_z) * 2 + core, "view": lax.rem(x + (code & 3), VIEWS)}

    def send(src, dst, sem_s, sem_r, device):
        return pltpu.make_async_remote_copy(
            src_ref=src, dst_ref=dst, send_sem=sem_s, recv_sem=sem_r, device_id=device,
            device_id_type=MESH,
        )

    barrier = pltpu.get_barrier_semaphore()

    def greet(j, carry):
        to = {"keys": lax.rem(k + j, OWNERS), "view": x}
        pl.semaphore_signal(barrier, inc=1, device_id=to, device_id_type=MESH)
        return carry

    with jax.named_scope("greet"):
        lax.fori_loop(1, OWNERS, greet, 0)
        for j in range(1, VIEWS):
            to = {"keys": k, "view": lax.rem(x + j, VIEWS)}
            pl.semaphore_signal(barrier, inc=1, device_id=to, device_id_type=MESH)
        for n in range(4, len(loads)):
            loads[n].start()

    with jax.named_scope("lookup_b"):
        for n in range(4):
            loads[n].wait()
        whole = key_slot[...]
        high = (whole >> 7).astype(F32).T
        low = (whole & 127).astype(F32).T
        table = jnp.concatenate([high, low], axis=0).astype(BF16)

        def look_up(r, key_ref, mult_ref, count_ref):
            slots, found, marks, ranks = places(table, key_ref, count_ref[0])
            for s in range(8):
                spot_ref[8 * r + s : 8 * r + s + 1, :] = found[s]
                sign_ref[8 * r + s : 8 * r + s + 1, :] = mult_ref[s : s + 1, :].astype(F32)
            return slots, marks, ranks

        slots_b, marks_b, ranks_b = look_up(0, db_key, db_mult, db_count)
        note = by_place(
            marks_b, ranks_b, [[v >> 4 for v in slots_b], [v & 15 for v in slots_b]]
        )
        note = (note[:OWNERS] * 16.0 + note[OWNERS:]).astype(I32)
        for n in range(OWNERS):
            db_info[n] = note[n : n + 1, :]

    def home(i):
        return lax.rem(OWNER_STEP * i, OWNERS)

    def owner_of(i):
        code = home(i)
        to_y, to_z = lax.rem(y + code // 8, 4), lax.rem(z + lax.rem(code // 2, 4), 4)
        return (to_y * 4 + to_z) * 2 + lax.rem(core + lax.rem(code, 2), 2)

    def packed(r, i, rows):
        at = iota((CAP, LANES), 0)
        picks = []
        for q in range(8):
            base = owner_of(8 * i + q) * CAP
            parts = []
            for s in range(8):
                spot = spot_ref[8 * r + s : 8 * r + s + 1, :]
                sign = sign_ref[8 * r + s : 8 * r + s + 1, :]
                parts.append(jnp.where(at == spot - base, sign, 0.0).astype(BF16))
            picks.append(jnp.concatenate(parts, axis=1))
        return dot(jnp.concatenate(picks, axis=0), rows[...]).astype(BF16)

    loads[4].wait()

    def pack_b(i, carry):
        blocks = packed(0, i, db_rows)
        for q in range(8):
            n = 8 * i + q
            for h in range(2):
                db_send[h, n] = blocks[q * CAP : (q + 1) * CAP, h * LANES : (h + 1) * LANES]
        return carry

    with jax.named_scope("pack_b"):
        lax.fori_loop(0, 4, pack_b, 0)

    with jax.named_scope("barrier"):
        pl.semaphore_wait(barrier, OWNERS - 1 + VIEWS - 1)

    def first_half(n, carry):
        to = {"keys": owner_of(n), "view": x}
        send(db_info.at[owner_of(n)], db_info_recv.at[home(n)], sems.at[0], sems.at[1], to).start()
        send(db_send.at[0, n], db_recv.at[0, home(n)], sems.at[2], sems.at[3], to).start()
        return carry

    def second_half(n, carry):
        to = {"keys": owner_of(n), "view": x}
        send(db_send.at[1, n], db_recv.at[1, home(n)], sems.at[4], sems.at[5], to).start()
        return carry

    with jax.named_scope("send_b"):
        lax.fori_loop(1, OWNERS, first_half, 0)
        for j in range(1, VIEWS):
            to = {"keys": k, "view": lax.rem(x + j, VIEWS)}
            pl.semaphore_signal(planes, inc=1, device_id=to, device_id_type=MESH)
        lax.fori_loop(1, OWNERS, second_half, 0)
    db_info_recv[0] = db_info[k]
    db_recv[0, 0] = db_send[0, 0]
    db_recv[1, 0] = db_send[1, 0]

    def eighth(at, part):
        return pl.ds(pl.multiple_of(at * 128 + part * 64, 64), 64)

    def quarter(at):
        return pl.ds(pl.multiple_of(at * 128, 128), 128)

    def across(part, got, s):
        for j in range(1, VIEWS):
            to = lax.rem(x + j, VIEWS)
            send(
                part.at[quarter(to)], got.at[j - 1], sems.at[s], sems.at[s + 1],
                {"keys": k, "view": to},
            ).start()

    def all_quarters(mine, full, s):
        for j in range(1, VIEWS):
            to = lax.rem(x + j, VIEWS)
            send(
                mine, full.at[quarter(x)], sems.at[s], sems.at[s + 1], {"keys": k, "view": to}
            ).start()

    for n in (5, 6, 7):
        loads[n].wait()
    with jax.named_scope("sum_b"):
        for m in range(2):
            acc = jnp.zeros((256, D), F32)
            for p in range(8):
                rows = [b_slot[4 * p + s : 4 * p + s + 1, :] for s in range(4)]
                values = [b_weight[4 * p + s : 4 * p + s + 1, :].astype(F32) for s in range(4)]
                hits = one_hot(rows, 256, 256 * m, values)
                acc = acc + dot(hits, b_rows[512 * p : 512 * (p + 1), :])
            part_b[256 * m : 256 * (m + 1), :] = acc
        across(part_b, got_b, 8)

    with jax.named_scope("lookup_a"):
        for n in range(8, 12):
            loads[n].wait()
        slots_a, marks_a, ranks_a = look_up(1, da_key, da_mult, da_count)
        groups = [da_group[s : s + 1, :] for s in range(8)]
        note = by_place(
            marks_a,
            ranks_a,
            [
                [v >> 4 for v in slots_a],
                [v & 15 for v in slots_a],
                [v >> 6 for v in groups],
                [v & 63 for v in groups],
            ],
        )
        slot_note = (note[:OWNERS] * 16.0 + note[OWNERS : 2 * OWNERS]).astype(I32)
        group_note = (note[2 * OWNERS : 3 * OWNERS] * 64.0 + note[3 * OWNERS :]).astype(I32)
        for n in range(OWNERS):
            da_info[n] = jnp.concatenate([slot_note[n : n + 1, :], group_note[n : n + 1, :]], axis=0)
    loads[12].wait()

    def pack_a(i, carry):
        blocks = packed(1, i, da_rows)
        for q in range(8):
            da_send[8 * i + q] = blocks[q * CAP : (q + 1) * CAP, :]
        return carry

    with jax.named_scope("pack_a"):
        lax.fori_loop(0, 4, pack_a, 0)

    def send_a_info(n, carry):
        to = {"keys": owner_of(n), "view": x}
        send(da_info.at[owner_of(n)], da_info_recv.at[home(n)], sems.at[6], sems.at[7], to).start()
        return carry

    lax.fori_loop(1, OWNERS, send_a_info, 0)
    da_info_recv[0] = da_info[k]
    da_recv[0] = da_send[0]

    left = iota((1, LANES), 1) < CAP

    def pair(ref, row, n):
        return jnp.where(left, ref[2 * n, row : row + 1, :], ref[2 * n + 1, row : row + 1, :])

    def sum_db(h):
        for m in range(2):
            acc = jnp.zeros((256, LANES), F32)
            for p in range(4):
                rows = [pair(db_info_recv, 0, 4 * p + s) for s in range(4)]
                blocks = db_recv[h, 8 * p : 8 * (p + 1)].reshape(512, LANES)
                acc = acc + dot(one_hot(rows, 256, 256 * m), blocks)
            part_db[h, 256 * m : 256 * (m + 1), :] = acc

    def finish_quarter(h):
        quarter_db[h] = part_db[h, quarter(x), :] + got_db[h, 0] + got_db[h, 1] + got_db[h, 2]
        all_quarters(quarter_db.at[h], full_db.at[h], 16 + 4 * h)
        full_db[h, quarter(x), :] = quarter_db[h]

    at_lane = iota((LANES, LANES), 1)

    def pick_block(j, carry):
        row = a_slot[pl.ds(j, 1), :] + KEYS_DEV * a_weight[pl.ds(j, 1), :]
        cols = jnp.broadcast_to(row.astype(F32), (LANES, LANES)).T.astype(I32)
        slot, weight = cols & (KEYS_DEV - 1), (cols >> 9).astype(F32)
        at = pl.ds(pl.multiple_of(j * LANES, LANES), LANES)
        for q in range(4):
            pick[at, q * LANES : (q + 1) * LANES] = jnp.where(
                at_lane + q * LANES == slot, weight, 0.0
            ).astype(BF16)
        return carry

    for n in (13, 14, 15):
        loads[n].wait()
    with jax.named_scope("pick"):
        lax.fori_loop(0, 32, pick_block, 0)

    def place(group):
        to_y, to_z, to_x = group >> 10, (group >> 8) & 3, (group >> 5) & 3
        code = ((to_y - y) & 3) * 16 + ((to_z - z) & 3) * 4 + ((to_x - x) & 3)
        rank = jnp.zeros_like(code)
        for n in range(PEERS):
            rank = jnp.where(code == n, RANK[n], rank)
        other = ((group >> 7) & 1) ^ core
        return other * HALF + rank * GROUPS_DEV + (group & 31)

    spots[0:32, :] = place(a_group[...])

    with jax.named_scope("wait_db0"):
        wait_bytes(db_info_recv.at[1:OWNERS], sems.at[1])
        wait_bytes(db_recv.at[0, 1:OWNERS], sems.at[3])
    sum_db(0)
    across(part_db.at[0], got_db.at[0], 14)

    with jax.named_scope("wait_b"):
        wait_bytes(got_b, sems.at[9])
    whole_b = part_b[quarter(x), :] + got_b[0] + got_b[1] + got_b[2]
    for h in range(2):
        quarter_b[h] = whole_b[:, h * LANES : (h + 1) * LANES]
        full_b[h, quarter(x), :] = quarter_b[h]
    all_quarters(quarter_b.at[0], full_b.at[0], 10)

    with jax.named_scope("wait_db1"):
        wait_bytes(db_recv.at[1, 1:OWNERS], sems.at[5])
    def send_a(n, carry):
        to = {"keys": owner_of(n), "view": x}
        send(da_send.at[n], da_recv.at[home(n)], sems.at[12], sems.at[13], to).start()
        return carry

    lax.fori_loop(1, OWNERS, send_a, 0)

    sum_db(1)
    for part in range(2):
        for j in range(1, VIEWS):
            to = lax.rem(x + j, VIEWS)
            send(
                part_db.at[1, eighth(to, part)], got_db.at[1, j - 1, 64 * part : 64 * part + 64],
                part_sems.at[part, 0], part_sems.at[part, 1], {"keys": k, "view": to},
            ).start()

    with jax.named_scope("wait_rs0"):
        wait_bytes(got_db.at[0], sems.at[15])
    finish_quarter(0)

    with jax.named_scope("wait_da_info"):
        wait_bytes(da_info_recv.at[1:OWNERS], sems.at[7])
    with jax.named_scope("pick_d"):
        groups_d = jnp.concatenate([pair(da_info_recv, 1, n) for n in range(16)], axis=0)
        spots[32:48, :] = place(groups_d)
        for n in range(16):
            cols = jnp.broadcast_to(
                pair(da_info_recv, 0, n).astype(F32), (LANES, LANES)
            ).T.astype(I32)
            for q in range(4):
                pick_d[n * LANES : (n + 1) * LANES, q * LANES : (q + 1) * LANES] = jnp.where(
                    at_lane + q * LANES == cols, 1.0, 0.0
                ).astype(BF16)

    def split(value):
        top = value.astype(BF16)
        return jnp.concatenate([top, (value - top.astype(F32)).astype(BF16)], axis=1)

    def a_terms(h):
        table_a[h] = split(full_db[h])

        def block(j, carry):
            at = pl.ds(pl.multiple_of(j * 2048, 2048), 2048)
            cut = slice(h * LANES, (h + 1) * LANES)
            both = dot(pick[at, :], table_a[h])
            value = (both[:, :LANES] + both[:, LANES:]) * a_rows[at, cut].astype(F32)
            terms[at, cut] = value.astype(BF16)
            return carry

        lax.fori_loop(0, 2, block, 0)

    for part in range(2):
        cut = slice(64 * part, 64 * part + 64)
        with jax.named_scope("wait_rs1"):
            wait_bytes(got_db.at[1, :, cut], part_sems.at[part, 1])
        quarter_db[1, cut] = (
            part_db[1, eighth(x, part), :]
            + got_db[1, 0, cut]
            + got_db[1, 1, cut]
            + got_db[1, 2, cut]
        )
        for j in range(1, VIEWS):
            to = lax.rem(x + j, VIEWS)
            send(
                quarter_db.at[1, cut], full_db.at[1, eighth(x, part)], sems.at[20], sems.at[21],
                {"keys": k, "view": to},
            ).start()
        full_db[1, eighth(x, part), :] = quarter_db[1, cut]
    all_quarters(quarter_b.at[1], full_b.at[1], 24)

    loads[16].wait()
    with jax.named_scope("wait_ag0"):
        wait_bytes(full_db.at[0, 0:384], sems.at[17])
    with jax.named_scope("a_terms0"):
        a_terms(0)

    with jax.named_scope("wait_ag1"):
        wait_bytes(full_db.at[1, 0:384], sems.at[21])
    with jax.named_scope("a_terms1"):
        a_terms(1)

    def base_of(t, steps):
        base = 0
        for n, (other, c) in enumerate(steps):
            base = jnp.where(t == n, other * HALF + CHUNKS[c][0], base)
        return base

    def summed(base, height, first, last):
        acc = jnp.zeros((height, D), F32)
        for p in range(first, last):
            rows = [spots[4 * p + s : 4 * p + s + 1, :] for s in range(4)]
            acc = acc + dot(one_hot(rows, height, base), terms[512 * p : 512 * (p + 1), :])
        return acc

    last = len(CHUNKS) - 1
    small_steps = [(1, 0), (1, last), (0, 0), (0, last)]
    big_steps = [(other, c) for c in range(1, last) for other in (1, 0)]

    def early_step(t, carry):
        early[t] = summed(base_of(t, small_steps), SMALL, 0, 8)
        return carry

    with jax.named_scope("early"):
        lax.fori_loop(0, EARLY, early_step, 0)

    with jax.named_scope("wait_ag_b"):
        wait_bytes(full_b.at[0, 0:384], sems.at[11])
        wait_bytes(full_b.at[1, 0:384], sems.at[25])
    for h in range(2):
        table_w[h] = split(full_db[h] + full_b[h])

    with jax.named_scope("wait_da"):
        wait_bytes(da_recv.at[1:OWNERS], sems.at[13])

    def d_block(j, carry):
        at = pl.ds(pl.multiple_of(j * 512, 512), 512)
        rows = da_recv[pl.ds(8 * j, 8)].reshape(512, D).astype(F32)
        for h in range(2):
            both = dot(pick_d[at, :], table_w[h])
            value = (both[:, :LANES] + both[:, LANES:]) * rows[:, h * LANES : (h + 1) * LANES]
            terms[
                pl.ds(pl.multiple_of(ROWS + j * 512, 512), 512), h * LANES : (h + 1) * LANES
            ] = value.astype(BF16)
        return carry

    with jax.named_scope("d_terms"):
        lax.fori_loop(0, 4, d_block, 0)

    def finish_step(t, some, held_sum):
        for n, other, c in some:
            start, size = CHUNKS[c]

            @pl.when(t == n)
            def _(other=other, c=c, start=start, size=size):
                rows = slice(start, start + size)
                if other:
                    near_send[rows] = held_sum[...]
                    send(
                        near_send.at[rows], near_recv.at[rows], near_sems.at[0, c],
                        near_sems.at[1, c], {"keys": partner, "view": x},
                    ).start()
                    return
                wait_bytes(near_recv.at[rows], near_sems.at[1, c])
                acc = held_sum[...] + near_recv[rows]
                if c == last:
                    own[...] = acc[size - GROUPS_DEV :, :]
                blocks = slice(start // GROUPS_DEV, (start + size) // GROUPS_DEV)
                far_send[blocks] = acc.astype(BF16).reshape(size // GROUPS_DEV, GROUPS_DEV, D)
                if c == 0:
                    pl.semaphore_wait(planes, VIEWS - 1)
                for m in range(blocks.start, blocks.stop):
                    code = FAR_FIRST[m]
                    if code:
                        send(
                            far_send.at[m], far_recv.at[code], sems.at[22], sems.at[23], peer(code)
                        ).start()

    def begun_step(t, carry):
        small_sum[...] = early[t] + summed(base_of(t, small_steps), SMALL, 8, 12)
        finish_step(t, [(n, *small_steps[n]) for n in range(EARLY)], small_sum)
        return carry

    def big_step(t, carry):
        big_sum[...] = summed(base_of(t, big_steps), CHUNK, 0, 12)
        finish_step(t, [(n, *step) for n, step in enumerate(big_steps)], big_sum)
        return carry

    def last_step(t, carry):
        small_sum[...] = summed(base_of(t, small_steps), SMALL, 0, 12)
        finish_step(t, [(n, *small_steps[n]) for n in range(EARLY, 4)], small_sum)
        return carry

    with jax.named_scope("begun"):
        lax.fori_loop(0, EARLY, begun_step, 0)
    with jax.named_scope("groups"):
        lax.fori_loop(0, len(big_steps), big_step, 0)
    with jax.named_scope("last"):
        lax.fori_loop(EARLY, 4, last_step, 0)

    with jax.named_scope("wait_far"):
        wait_bytes(far_recv.at[1:PEERS], sems.at[23])
    with jax.named_scope("tail"):
        total = own[...]
        for j in range(1, PEERS):
            total = total + far_recv[j].astype(F32)
        out[...] = total

    wait_bytes(db_info.at[1:OWNERS], sems.at[0])
    wait_bytes(db_send.at[0, 1:OWNERS], sems.at[2])
    wait_bytes(db_send.at[1, 1:OWNERS], sems.at[4])
    wait_bytes(da_info.at[1:OWNERS], sems.at[6])
    wait_bytes(part_b.at[0:384], sems.at[8])
    wait_bytes(full_b.at[0, 0:384], sems.at[10])
    wait_bytes(full_b.at[1, 0:384], sems.at[24])
    wait_bytes(da_send.at[1:OWNERS], sems.at[12])
    for h in range(2):
        wait_bytes(part_db.at[h, 0:384], sems.at[16 + 4 * h])
        wait_bytes(got_db.at[1, :, 0:64], part_sems.at[h, 0])
    wait_bytes(part_db.at[0, 0:384], sems.at[14])
    wait_bytes(far_send.at[0 : PEERS - 1], sems.at[22])
    for c, (start, size) in enumerate(CHUNKS):
        wait_bytes(near_send.at[start : start + size], near_sems.at[0, c])


def shards(
    key_slot, a_slot, a_group, a_weight, a_payload, b_slot, b_weight, b_payload, da_key, da_group,
    da_mult, da_payload, da_count, db_key, db_mult, db_payload, db_count,
):
    vmem = pl.BlockSpec(memory_space=pltpu.VMEM)
    hbm = pl.BlockSpec(memory_space=pl.ANY)

    def lanes(v):
        return v.reshape(-1, LANES)

    def held(*shape, dtype=F32):
        return pltpu.VMEM(shape, dtype)

    return pl.pallas_call(
        kernel,
        out_shape=jax.ShapeDtypeStruct((GROUPS_DEV, D), F32),
        in_specs=[hbm] * 17,
        out_specs=vmem,
        scratch_shapes=[
            held(LANES, LANES, dtype=I32),
            held(8, LANES, dtype=I32),
            held(8, LANES, dtype=I32),
            held(32, LANES, dtype=I32),
            held(32, LANES, dtype=I32),
            held(8, LANES, dtype=I32),
            held(8, LANES, dtype=I32),
            held(8, LANES, dtype=I32),
            held(32, LANES, dtype=I32),
            held(32, LANES, dtype=I32),
            held(32, LANES, dtype=I32),
            pltpu.SMEM((1,), I32),
            pltpu.SMEM((1,), I32),
            held(DELTA, D, dtype=BF16),
            held(DELTA, D, dtype=BF16),
            held(ROWS, D, dtype=BF16),
            held(ROWS, D, dtype=BF16),
            held(16, LANES, dtype=I32),
            held(16, LANES),
            held(2, OWNERS, CAP, LANES, dtype=BF16),
            held(OWNERS, CAP, D, dtype=BF16),
            held(OWNERS, 1, LANES, dtype=I32),
            held(OWNERS, 2, LANES, dtype=I32),
            held(2, OWNERS, CAP, LANES, dtype=BF16),
            held(OWNERS, CAP, D, dtype=BF16),
            held(OWNERS, 1, LANES, dtype=I32),
            held(OWNERS, 2, LANES, dtype=I32),
            held(KEYS_DEV, D),
            held(2, 128, LANES),
            held(3, 128, D),
            held(2, KEYS_DEV, LANES),
            held(2, KEYS_DEV, LANES),
            held(2, 128, LANES),
            held(2, 3, 128, LANES),
            held(2, KEYS_DEV, LANES),
            held(ROWS, KEYS_DEV, dtype=BF16),
            held(OWNERS * CAP, KEYS_DEV, dtype=BF16),
            held(2, KEYS_DEV, D, dtype=BF16),
            held(2, KEYS_DEV, D, dtype=BF16),
            held(ROWS + OWNERS * CAP, D, dtype=BF16),
            held(48, LANES, dtype=I32),
            held(HALF, D),
            held(HALF, D),
            held(PEERS, GROUPS_DEV, D, dtype=BF16),
            held(PEERS, GROUPS_DEV, D, dtype=BF16),
            held(GROUPS_DEV, D),
            held(CHUNK, D),
            held(SMALL, D),
            held(EARLY, SMALL, D),
            pltpu.SemaphoreType.DMA((17,)),
            pltpu.SemaphoreType.DMA((26,)),
            pltpu.SemaphoreType.DMA((2, len(CHUNKS))),
            pltpu.SemaphoreType.DMA((2, 2)),
            pltpu.SemaphoreType.REGULAR,
        ],
        compiler_params=pltpu.CompilerParams(
            collective_id=0, has_side_effects=True, vmem_limit_bytes=56 * 1024 * 1024
        ),
    )(
        lanes(key_slot), lanes(db_key), lanes(db_mult), db_count, db_payload, lanes(b_slot),
        lanes(b_weight), b_payload, lanes(da_key), lanes(da_group), lanes(da_mult), da_count,
        da_payload, lanes(a_slot), lanes(a_weight), lanes(a_group), a_payload,
    )


def solution(mesh):
    rows = P(("keys", "view"))
    wide = P(("keys", "view"), None)
    placed = (
        P(), rows, rows, rows, wide, rows, rows, wide, rows, rows, rows, wide, rows, rows, rows,
        wide, rows,
    )
    return jax.shard_map(
        shards, mesh=mesh, in_specs=placed, out_specs=wide, check_vma=False
    )
```

```python
import jax
import jax.numpy as jnp
from jax import lax
from jax.experimental import pallas as pl
from jax.experimental.pallas import tpu as pltpu
from jax.sharding import PartitionSpec as P

MESH = pl.DeviceIdType.MESH
F32, BF16, I32 = jnp.float32, jnp.bfloat16, jnp.int32
D = 256
KEYS_DEV = 512
GROUPS_DEV = 32
ROWS = 4096
DELTA = 1024
CAP = 64
OWNERS = 32
VIEWS = 4
LANES = 128
PEERS = 64
HALF = 2048
CHUNK = 512


def apart(code):
    return sum((0, 1, 2, 1)[d] for d in (code >> 4, (code >> 2) & 3, code & 3))


FAR_FIRST = sorted(range(PEERS), key=lambda code: (-apart(code), (code * 27) % PEERS))
OWNERS_MIXED = [11 * n % OWNERS for n in range(1, OWNERS)]
RANK = [FAR_FIRST.index(code) for code in range(PEERS)]


def iota(shape, dim):
    return lax.broadcasted_iota(I32, shape, dim)


def dot(a, b):
    return jnp.dot(a, b, preferred_element_type=F32)


def one_hot(rows, height, base, values=None):
    at = iota((height, LANES), 0)
    parts = []
    for n, row in enumerate(rows):
        value = 1.0 if values is None else values[n]
        parts.append(jnp.where(at == row - base, value, 0.0).astype(BF16))
    return jnp.concatenate(parts, axis=1)


def places(table, key_ref, count):
    keys = [key_ref[s : s + 1, :] for s in range(DELTA // LANES)]
    at = iota((LANES, LANES), 0)
    hits = jnp.concatenate(
        [jnp.where(at == (k >> 7), 1.0, 0.0).astype(BF16) for k in keys], axis=1
    )
    found = dot(table, hits)
    slots, owners, lives, marks = [], [], [], []
    lane = iota((1, LANES), 1)
    owner_at = iota((OWNERS, LANES), 0)
    for s, k in enumerate(keys):
        cut = slice(s * LANES, (s + 1) * LANES)
        value = found[:LANES, cut] * 128.0 + found[LANES:, cut]
        slot = jnp.sum(jnp.where(at == (k & 127), value, 0.0), axis=0, keepdims=True).astype(I32)
        live = lane + s * LANES < count
        owner = jnp.where(live, slot >> 9, -1)
        slots.append(slot & (KEYS_DEV - 1))
        owners.append(owner)
        lives.append(live)
        marks.append(jnp.where(owner_at == owner, 1.0, 0.0))
    stacked = jnp.concatenate(marks, axis=0).astype(BF16)
    col = iota((LANES, 2 * LANES), 1)
    before = jnp.where((iota((LANES, 2 * LANES), 0) < col) | (col >= LANES), 1.0, 0.0).astype(BF16)
    counts = dot(stacked, before)
    carry = jnp.zeros((OWNERS, LANES), F32)
    spots, ranks = [], []
    for s in range(len(keys)):
        cut = slice(s * OWNERS, (s + 1) * OWNERS)
        rank = jnp.sum(marks[s] * (counts[cut, :LANES] + carry), axis=0, keepdims=True).astype(I32)
        ranks.append(rank)
        spots.append(jnp.where(lives[s], owners[s] * CAP + rank, -1))
        carry = carry + counts[cut, LANES:]
    return slots, spots, marks, ranks


def by_place(marks, ranks, values):
    rank_at = iota((LANES, LANES), 0) & (CAP - 1)
    there = jnp.concatenate(
        [jnp.where(rank_at == rank, 1.0, 0.0).astype(BF16) for rank in ranks], axis=1
    )
    rows = jnp.concatenate(
        [
            jnp.concatenate([mark * v.astype(F32) for mark, v in zip(marks, value)], axis=1)
            for value in values
        ],
        axis=0,
    ).astype(BF16)
    return lax.dot_general(rows, there, (((1,), (1,)), ((), ())), preferred_element_type=F32)


def wait_bytes(ref, sem):
    pltpu.make_async_copy(ref, ref, sem).wait()


def kernel(
    key_slot_hbm, db_key_hbm, db_mult_hbm, db_count_hbm, db_hbm, b_slot_hbm, b_weight_hbm, b_hbm,
    da_key_hbm, da_group_hbm, da_mult_hbm, da_count_hbm, da_hbm, a_slot_hbm, a_weight_hbm,
    a_group_hbm, a_hbm,
    out,
    key_slot, db_key, db_mult, b_slot, b_weight, da_key, da_group, da_mult, a_slot, a_weight,
    a_group, da_count, db_count, da_rows, db_rows, b_rows, a_rows, spot_ref, sign_ref,
    db_send, da_send, db_info, da_info, db_recv, da_recv, db_info_recv, da_info_recv,
    part_b, quarter_b, got_b, full_b, part_db, quarter_db, got_db, full_db,
    pick, pick_d, table_a, table_w, terms, spots, near_send, near_recv, far_send, far_recv, own, chunk_sum, part_sum,
    spot_cols, a_turned, a_term,
    load_sems, sems, near_sems, part_sems, far_sems, planes,
):
    k, x = lax.axis_index("keys"), lax.axis_index("view")
    core = lax.rem(k, 2)
    partner = k + 1 - 2 * core
    y, z = k // 8, lax.rem(k // 2, 4)

    pairs = (
        (key_slot_hbm, key_slot), (db_key_hbm, db_key), (db_mult_hbm, db_mult),
        (db_count_hbm, db_count), (db_hbm, db_rows), (b_slot_hbm, b_slot),
        (b_weight_hbm, b_weight), (b_hbm, b_rows), (da_key_hbm, da_key),
        (da_group_hbm, da_group), (da_mult_hbm, da_mult), (da_count_hbm, da_count),
        (da_hbm, da_rows), (a_slot_hbm, a_slot), (a_weight_hbm, a_weight),
        (a_group_hbm, a_group), (a_hbm, a_rows),
    )
    loads = [
        pltpu.make_async_copy(src, dst, load_sems.at[n]) for n, (src, dst) in enumerate(pairs)
    ]
    for n in range(4):
        loads[n].start()

    def peer(code):
        to_y, to_z = lax.rem(y + (code >> 4), 4), lax.rem(z + ((code >> 2) & 3), 4)
        return {"keys": (to_y * 4 + to_z) * 2 + core, "view": lax.rem(x + (code & 3), VIEWS)}

    def send(src, dst, sem_s, sem_r, device):
        return pltpu.make_async_remote_copy(
            src_ref=src, dst_ref=dst, send_sem=sem_s, recv_sem=sem_r, device_id=device,
            device_id_type=MESH,
        )

    barrier = pltpu.get_barrier_semaphore()

    def greet(j, carry):
        to = {"keys": lax.rem(k + j, OWNERS), "view": x}
        pl.semaphore_signal(barrier, inc=1, device_id=to, device_id_type=MESH)
        return carry

    with jax.named_scope("greet"):
        lax.fori_loop(1, OWNERS, greet, 0)
        for j in range(1, VIEWS):
            to = {"keys": k, "view": lax.rem(x + j, VIEWS)}
            pl.semaphore_signal(barrier, inc=1, device_id=to, device_id_type=MESH)
        for n in range(4, len(loads)):
            loads[n].start()

    with jax.named_scope("lookup_b"):
        for n in range(4):
            loads[n].wait()
        whole = key_slot[...]
        high = (whole >> 7).astype(F32).T
        low = (whole & 127).astype(F32).T
        table = jnp.concatenate([high, low], axis=0).astype(BF16)

        def look_up(r, key_ref, mult_ref, count_ref):
            slots, found, marks, ranks = places(table, key_ref, count_ref[0])
            for s in range(8):
                spot_ref[8 * r + s : 8 * r + s + 1, :] = found[s]
                sign_ref[8 * r + s : 8 * r + s + 1, :] = mult_ref[s : s + 1, :].astype(F32)
            return slots, marks, ranks

        slots_b, marks_b, ranks_b = look_up(0, db_key, db_mult, db_count)
        note = by_place(
            marks_b, ranks_b, [[v >> 4 for v in slots_b], [v & 15 for v in slots_b]]
        )
        note = (note[:OWNERS] * 16.0 + note[OWNERS:]).astype(I32)
        for n in range(OWNERS):
            db_info[n] = note[n : n + 1, :]

    def owner_of(code):
        to_y, to_z = lax.rem(y + code // 8, 4), lax.rem(z + (code // 2) % 4, 4)
        return (to_y * 4 + to_z) * 2 + lax.rem(core + code % 2, 2)

    def packed(r, i, rows):
        spots = [spot_ref[8 * r + s : 8 * r + s + 1, :] for s in range(8)]
        signs = [sign_ref[8 * r + s : 8 * r + s + 1, :] for s in range(8)]
        return dot(one_hot(spots, 512, 512 * i, signs), rows[...]).astype(BF16)

    loads[4].wait()

    def pack_b(i, carry):
        blocks = packed(0, i, db_rows).reshape(8, CAP, D)
        for h in range(2):
            db_send[h, pl.ds(8 * i, 8)] = blocks[:, :, h * LANES : (h + 1) * LANES]
        return carry

    with jax.named_scope("pack_b"):
        lax.fori_loop(0, 4, pack_b, 0)

    with jax.named_scope("barrier"):
        pl.semaphore_wait(barrier, OWNERS - 1 + VIEWS - 1)

    with jax.named_scope("send_b"):
        for code in OWNERS_MIXED:
            n = owner_of(code)
            to = {"keys": n, "view": x}
            send(db_info.at[n], db_info_recv.at[code], sems.at[0], sems.at[1], to).start()
            send(db_send.at[0, n], db_recv.at[0, code], sems.at[2], sems.at[3], to).start()
        for code in OWNERS_MIXED:
            n = owner_of(code)
            to = {"keys": n, "view": x}
            send(db_send.at[1, n], db_recv.at[1, code], sems.at[4], sems.at[5], to).start()
        for j in range(1, VIEWS):
            to = {"keys": k, "view": lax.rem(x + j, VIEWS)}
            pl.semaphore_signal(planes, inc=1, device_id=to, device_id_type=MESH)
    db_info_recv[0] = db_info[k]
    db_recv[0, 0] = db_send[0, k]
    db_recv[1, 0] = db_send[1, k]

    def eighth(at, part):
        return pl.ds(pl.multiple_of(at * 128 + part * 64, 64), 64)

    def quarter(at):
        return pl.ds(pl.multiple_of(at * 128, 128), 128)

    def across(part, got, s):
        for j in range(1, VIEWS):
            to = lax.rem(x + j, VIEWS)
            send(
                part.at[quarter(to)], got.at[j - 1], sems.at[s], sems.at[s + 1],
                {"keys": k, "view": to},
            ).start()

    def all_quarters(mine, full, s):
        for j in range(1, VIEWS):
            to = lax.rem(x + j, VIEWS)
            send(
                mine, full.at[quarter(x)], sems.at[s], sems.at[s + 1], {"keys": k, "view": to}
            ).start()

    for n in (5, 6, 7):
        loads[n].wait()
    with jax.named_scope("sum_b"):
        for m in range(2):
            acc = jnp.zeros((256, D), F32)
            for p in range(8):
                rows = [b_slot[4 * p + s : 4 * p + s + 1, :] for s in range(4)]
                values = [b_weight[4 * p + s : 4 * p + s + 1, :].astype(F32) for s in range(4)]
                hits = one_hot(rows, 256, 256 * m, values)
                acc = acc + dot(hits, b_rows[512 * p : 512 * (p + 1), :])
            part_b[256 * m : 256 * (m + 1), :] = acc
        across(part_b, got_b, 8)

    with jax.named_scope("lookup_a"):
        for n in range(8, 12):
            loads[n].wait()
        slots_a, marks_a, ranks_a = look_up(1, da_key, da_mult, da_count)
        groups = [da_group[s : s + 1, :] for s in range(8)]
        note = by_place(
            marks_a,
            ranks_a,
            [
                [v >> 4 for v in slots_a],
                [v & 15 for v in slots_a],
                [v >> 6 for v in groups],
                [v & 63 for v in groups],
            ],
        )
        slot_note = (note[:OWNERS] * 16.0 + note[OWNERS : 2 * OWNERS]).astype(I32)
        group_note = (note[2 * OWNERS : 3 * OWNERS] * 64.0 + note[3 * OWNERS :]).astype(I32)
        for n in range(OWNERS):
            da_info[n] = jnp.concatenate([slot_note[n : n + 1, :], group_note[n : n + 1, :]], axis=0)
    loads[12].wait()

    def pack_a(i, carry):
        da_send[pl.ds(8 * i, 8)] = packed(1, i, da_rows).reshape(8, CAP, D)
        return carry

    with jax.named_scope("pack_a"):
        lax.fori_loop(0, 4, pack_a, 0)

    for code in OWNERS_MIXED:
        n = owner_of(code)
        to = {"keys": n, "view": x}
        send(da_info.at[n], da_info_recv.at[code], sems.at[6], sems.at[7], to).start()
    da_info_recv[0] = da_info[k]
    da_recv[0] = da_send[k]

    left = iota((1, LANES), 1) < CAP

    def pair(ref, row, n):
        return jnp.where(left, ref[2 * n, row : row + 1, :], ref[2 * n + 1, row : row + 1, :])

    def sum_db(h):
        for m in range(2):
            acc = jnp.zeros((256, LANES), F32)
            for p in range(4):
                rows = [pair(db_info_recv, 0, 4 * p + s) for s in range(4)]
                blocks = db_recv[h, 8 * p : 8 * (p + 1)].reshape(512, LANES)
                acc = acc + dot(one_hot(rows, 256, 256 * m), blocks)
            part_db[h, 256 * m : 256 * (m + 1), :] = acc

    def finish_quarter(h):
        quarter_db[h] = part_db[h, quarter(x), :] + got_db[h, 0] + got_db[h, 1] + got_db[h, 2]
        all_quarters(quarter_db.at[h], full_db.at[h], 16 + 4 * h)
        full_db[h, quarter(x), :] = quarter_db[h]

    at_lane = iota((LANES, LANES), 1)

    def place(group):
        to_y, to_z, to_x = group >> 10, (group >> 8) & 3, (group >> 5) & 3
        code = ((to_y - y) & 3) * 16 + ((to_z - z) & 3) * 4 + ((to_x - x) & 3)
        rank = jnp.zeros_like(code)
        for n in range(PEERS):
            rank = jnp.where(code == n, RANK[n], rank)
        other = ((group >> 7) & 1) ^ core
        return other * HALF + rank * GROUPS_DEV + (group & 31)

    for n in range(13, 17):
        loads[n].wait()
    with jax.named_scope("pick"):
        spots[0:32, :] = place(a_group[...])

        def pick_block(j, carry):
            at = pl.ds(pl.multiple_of(j * LANES, LANES), LANES)
            value = a_weight[pl.ds(j, 1), :].astype(F32)
            pick[:, at] = one_hot([a_slot[pl.ds(j, 1), :]], KEYS_DEV, 0, [value])
            row = jnp.broadcast_to(spots[pl.ds(j, 1), :].astype(F32), (LANES, LANES))
            spot_cols[at, :] = row.T.astype(I32) - at_lane
            turned = a_rows[at, :].astype(F32).T.astype(BF16)
            for h in range(2):
                a_turned[h, :, at] = turned[h * LANES : (h + 1) * LANES, :]
            return carry

        lax.fori_loop(0, 32, pick_block, 0)

    with jax.named_scope("wait_db0"):
        wait_bytes(db_info_recv.at[1:OWNERS], sems.at[1])
        wait_bytes(db_recv.at[0, 1:OWNERS], sems.at[3])
    sum_db(0)
    across(part_db.at[0], got_db.at[0], 14)

    with jax.named_scope("wait_b"):
        wait_bytes(got_b, sems.at[9])
    whole_b = part_b[quarter(x), :] + got_b[0] + got_b[1] + got_b[2]
    for h in range(2):
        quarter_b[h] = whole_b[:, h * LANES : (h + 1) * LANES]
        full_b[h, quarter(x), :] = quarter_b[h]

    with jax.named_scope("wait_db1"):
        wait_bytes(db_recv.at[1, 1:OWNERS], sems.at[5])
    for code in OWNERS_MIXED:
        n = owner_of(code)
        to = {"keys": n, "view": x}
        send(da_send.at[n], da_recv.at[code], sems.at[12], sems.at[13], to).start()
    sum_db(1)
    for part in range(2):
        for j in range(1, VIEWS):
            to = lax.rem(x + j, VIEWS)
            send(
                part_db.at[1, eighth(to, part)], got_db.at[1, j - 1, 64 * part : 64 * part + 64],
                part_sems.at[part, 0], part_sems.at[part, 1], {"keys": k, "view": to},
            ).start()

    with jax.named_scope("wait_rs0"):
        wait_bytes(got_db.at[0], sems.at[15])
    finish_quarter(0)


    with jax.named_scope("wait_da_info"):
        wait_bytes(da_info_recv.at[1:OWNERS], sems.at[7])
    with jax.named_scope("pick_d"):
        groups_d = jnp.concatenate([pair(da_info_recv, 1, n) for n in range(16)], axis=0)
        spots[32:48, :] = place(groups_d)
        for n in range(16):
            cols = jnp.broadcast_to(
                pair(da_info_recv, 0, n).astype(F32), (LANES, LANES)
            ).T.astype(I32)
            for q in range(4):
                pick_d[n * LANES : (n + 1) * LANES, q * LANES : (q + 1) * LANES] = jnp.where(
                    at_lane + q * LANES == cols, 1.0, 0.0
                ).astype(BF16)

    def split(value):
        top = value.astype(BF16)
        return jnp.concatenate([top, (value - top.astype(F32)).astype(BF16)], axis=1)

    def a_terms(h):
        flat = full_db[h].T
        top = flat.astype(BF16)
        table_a[...] = jnp.concatenate([top, (flat - top.astype(F32)).astype(BF16)], axis=0)

        def block(j, carry):
            at = pl.ds(pl.multiple_of(j * 2048, 2048), 2048)
            both = dot(table_a[...], pick[:, at])
            value = (both[:LANES] + both[LANES:]) * a_turned[h, :, at].astype(F32)
            a_term[h, :, at] = value.astype(BF16)
            return carry

        lax.fori_loop(0, 2, block, 0)

    def pick_base(t, bases):
        base = 0
        for n, value in enumerate(bases):
            base = jnp.where(t == n, value, base)
        return base

    def a_sum(h, base, width):
        acc = jnp.zeros((LANES, width), F32)
        for p in range(16):
            at = slice(256 * p, 256 * (p + 1))
            cols = spot_cols[at, :] - base
            hits = jnp.concatenate(
                [
                    jnp.where(cols == q * LANES, 1.0, 0.0).astype(BF16)
                    for q in range(width // LANES)
                ],
                axis=1,
            )
            acc = acc + dot(a_term[h, :, at], hits)
        return acc.T

    def a_sums(h, bases, width=1024):
        def block(t, carry):
            base = pl.multiple_of(pick_base(t, bases), width)
            part_sum[pl.ds(base, width), h * LANES : (h + 1) * LANES] = a_sum(h, base, width)
            return carry

        lax.fori_loop(0, len(bases), block, 0)

    for part in range(2):
        cut = slice(64 * part, 64 * part + 64)
        with jax.named_scope("wait_rs1"):
            wait_bytes(got_db.at[1, :, cut], part_sems.at[part, 1])
        quarter_db[1, cut] = (
            part_db[1, eighth(x, part), :]
            + got_db[1, 0, cut]
            + got_db[1, 1, cut]
            + got_db[1, 2, cut]
        )
        for j in range(1, VIEWS):
            to = lax.rem(x + j, VIEWS)
            send(
                quarter_db.at[1, cut], full_db.at[1, eighth(x, part)], sems.at[20], sems.at[21],
                {"keys": k, "view": to},
            ).start()
        full_db[1, eighth(x, part), :] = quarter_db[1, cut]

    for h in range(2):
        all_quarters(quarter_b.at[h], full_b.at[h], 10 + 14 * h)
    with jax.named_scope("wait_ag0"):
        wait_bytes(full_db.at[0, 0:384], sems.at[17])
    with jax.named_scope("a_terms0"):
        a_terms(0)
    with jax.named_scope("a_sums0b"):
        a_sums(0, [HALF, 0])
    with jax.named_scope("wait_ag1"):
        wait_bytes(full_db.at[1, 0:384], sems.at[21])
    with jax.named_scope("a_terms1"):
        a_terms(1)
    with jax.named_scope("a_sums1a"):
        a_sums(1, [HALF, HALF + CHUNK], CHUNK)

    with jax.named_scope("wait_ag_b"):
        wait_bytes(full_b.at[0, 0:384], sems.at[11])
        wait_bytes(full_b.at[1, 0:384], sems.at[25])
    for h in range(2):
        table_w[h] = split(full_db[h] + full_b[h])

    with jax.named_scope("wait_da"):
        wait_bytes(da_recv.at[1:OWNERS], sems.at[13])

    def d_block(j, carry):
        at = pl.ds(pl.multiple_of(j * 1024, 1024), 1024)
        rows = da_recv[pl.ds(16 * j, 16)].reshape(1024, D).astype(F32)
        for h in range(2):
            both = dot(pick_d[at, :], table_w[h])
            value = (both[:, :LANES] + both[:, LANES:]) * rows[:, h * LANES : (h + 1) * LANES]
            terms[at, h * LANES : (h + 1) * LANES] = value.astype(BF16)
        return carry

    with jax.named_scope("d_terms"):
        lax.fori_loop(0, 2, d_block, 0)

    def to_partner(c):
        rows = slice(c * CHUNK, (c + 1) * CHUNK)
        near_send[rows] = chunk_sum[...]
        send(
            near_send.at[rows], near_recv.at[rows], near_sems.at[0, c], near_sems.at[1, c],
            {"keys": partner, "view": x},
        ).start()

    def to_groups(c):
        rows = slice(c * CHUNK, (c + 1) * CHUNK)
        blocks = range(c * CHUNK // GROUPS_DEV, (c + 1) * CHUNK // GROUPS_DEV)
        wait_bytes(near_recv.at[rows], near_sems.at[1, c])
        acc = chunk_sum[...] + near_recv[rows]
        if blocks.stop == PEERS:
            own[...] = acc[CHUNK - GROUPS_DEV :, :]
        far_send[blocks.start : blocks.stop] = acc.astype(BF16).reshape(
            len(blocks), GROUPS_DEV, D
        )
        if c == 0:
            pl.semaphore_wait(planes, VIEWS - 1)
        for m in blocks:
            code = FAR_FIRST[m]
            if code:
                send(
                    far_send.at[m], far_recv.at[m], sems.at[22], far_sems.at[c], peer(code)
                ).start()

    def d_sum(base):
        acc = jnp.zeros((CHUNK, D), F32)
        for p in range(4):
            rows = [spots[32 + 4 * p + s : 33 + 4 * p + s, :] for s in range(4)]
            acc = acc + dot(one_hot(rows, CHUNK, base), terms[512 * p : 512 * (p + 1), :])
        return acc

    def sums(steps, begun):
        def block(t, carry):
            base = pick_base(t, [other * HALF + c * CHUNK for other, c in steps])
            base = pl.multiple_of(base, CHUNK)
            at = pl.ds(base, CHUNK)
            if begun:
                chunk_sum[...] = d_sum(base) + part_sum[at, :]
            else:
                turned = a_sum(1, base, CHUNK)
                acc = d_sum(base)
                chunk_sum[:, :LANES] = acc[:, :LANES] + part_sum[at, :LANES]
                chunk_sum[:, LANES:] = acc[:, LANES:] + turned
            for n, (other, c) in enumerate(steps):
                pl.when(t == n)(lambda other=other, c=c: (to_partner if other else to_groups)(c))
            return carry

        lax.fori_loop(0, len(steps), block, 0)

    with jax.named_scope("sums1"):
        sums([(1, 0), (1, 1)], True)
    with jax.named_scope("sums2"):
        sums([(0, 0), (0, 1)], False)
    with jax.named_scope("sums3"):
        a_sums(0, [HALF + 1024])
        sums([(1, 2), (1, 3)], False)
    with jax.named_scope("sums4"):
        a_sums(0, [1024])
        sums([(0, 2), (0, 3)], False)

    total = own[...]
    for c in range(HALF // CHUNK):
        first, stop = c * CHUNK // GROUPS_DEV, min((c + 1) * CHUNK // GROUPS_DEV, PEERS - 1)
        with jax.named_scope("wait_far" if stop == PEERS - 1 else "arrive"):
            wait_bytes(far_recv.at[first:stop], far_sems.at[c])
        for m in range(first, stop):
            total = total + far_recv[m].astype(F32)
    out[...] = total

    wait_bytes(db_info.at[1:OWNERS], sems.at[0])
    wait_bytes(db_send.at[0, 1:OWNERS], sems.at[2])
    wait_bytes(db_send.at[1, 1:OWNERS], sems.at[4])
    wait_bytes(da_info.at[1:OWNERS], sems.at[6])
    wait_bytes(part_b.at[0:384], sems.at[8])
    wait_bytes(full_b.at[0, 0:384], sems.at[10])
    wait_bytes(full_b.at[1, 0:384], sems.at[24])
    wait_bytes(da_send.at[1:OWNERS], sems.at[12])
    for h in range(2):
        wait_bytes(part_db.at[h, 0:384], sems.at[16 + 4 * h])
        wait_bytes(got_db.at[1, :, 0:64], part_sems.at[h, 0])
    wait_bytes(part_db.at[0, 0:384], sems.at[14])
    wait_bytes(far_send.at[0 : PEERS - 1], sems.at[22])
    for c in range(HALF // CHUNK):
        wait_bytes(near_send.at[c * CHUNK : (c + 1) * CHUNK], near_sems.at[0, c])


def shards(
    key_slot, a_slot, a_group, a_weight, a_payload, b_slot, b_weight, b_payload, da_key, da_group,
    da_mult, da_payload, da_count, db_key, db_mult, db_payload, db_count,
):
    vmem = pl.BlockSpec(memory_space=pltpu.VMEM)
    hbm = pl.BlockSpec(memory_space=pl.ANY)

    def lanes(v):
        return v.reshape(-1, LANES)

    def held(*shape, dtype=F32):
        return pltpu.VMEM(shape, dtype)

    return pl.pallas_call(
        kernel,
        out_shape=jax.ShapeDtypeStruct((GROUPS_DEV, D), F32),
        in_specs=[hbm] * 17,
        out_specs=vmem,
        scratch_shapes=[
            held(LANES, LANES, dtype=I32),
            held(8, LANES, dtype=I32),
            held(8, LANES, dtype=I32),
            held(32, LANES, dtype=I32),
            held(32, LANES, dtype=I32),
            held(8, LANES, dtype=I32),
            held(8, LANES, dtype=I32),
            held(8, LANES, dtype=I32),
            held(32, LANES, dtype=I32),
            held(32, LANES, dtype=I32),
            held(32, LANES, dtype=I32),
            pltpu.SMEM((1,), I32),
            pltpu.SMEM((1,), I32),
            held(DELTA, D, dtype=BF16),
            held(DELTA, D, dtype=BF16),
            held(ROWS, D, dtype=BF16),
            held(ROWS, D, dtype=BF16),
            held(16, LANES, dtype=I32),
            held(16, LANES),
            held(2, OWNERS, CAP, LANES, dtype=BF16),
            held(OWNERS, CAP, D, dtype=BF16),
            held(OWNERS, 1, LANES, dtype=I32),
            held(OWNERS, 2, LANES, dtype=I32),
            held(2, OWNERS, CAP, LANES, dtype=BF16),
            held(OWNERS, CAP, D, dtype=BF16),
            held(OWNERS, 1, LANES, dtype=I32),
            held(OWNERS, 2, LANES, dtype=I32),
            held(KEYS_DEV, D),
            held(2, 128, LANES),
            held(3, 128, D),
            held(2, KEYS_DEV, LANES),
            held(2, KEYS_DEV, LANES),
            held(2, 128, LANES),
            held(2, 3, 128, LANES),
            held(2, KEYS_DEV, LANES),
            held(KEYS_DEV, ROWS, dtype=BF16),
            held(OWNERS * CAP, KEYS_DEV, dtype=BF16),
            held(D, KEYS_DEV, dtype=BF16),
            held(2, KEYS_DEV, D, dtype=BF16),
            held(OWNERS * CAP, D, dtype=BF16),
            held(48, LANES, dtype=I32),
            held(HALF, D),
            held(HALF, D),
            held(PEERS, GROUPS_DEV, D, dtype=BF16),
            held(PEERS, GROUPS_DEV, D, dtype=BF16),
            held(GROUPS_DEV, D),
            held(CHUNK, D),
            held(PEERS * 2 * GROUPS_DEV, D),
            held(ROWS, LANES, dtype=I32),
            held(2, LANES, ROWS, dtype=BF16),
            held(2, LANES, ROWS, dtype=BF16),
            pltpu.SemaphoreType.DMA((17,)),
            pltpu.SemaphoreType.DMA((26,)),
            pltpu.SemaphoreType.DMA((2, HALF // CHUNK)),
            pltpu.SemaphoreType.DMA((2, 2)),
            pltpu.SemaphoreType.DMA((HALF // CHUNK,)),
            pltpu.SemaphoreType.REGULAR,
        ],
        compiler_params=pltpu.CompilerParams(
            collective_id=0, has_side_effects=True, vmem_limit_bytes=56 * 1024 * 1024
        ),
    )(
        lanes(key_slot), lanes(db_key), lanes(db_mult), db_count, db_payload, lanes(b_slot),
        lanes(b_weight), b_payload, lanes(da_key), lanes(da_group), lanes(da_mult), da_count,
        da_payload, lanes(a_slot), lanes(a_weight), lanes(a_group), a_payload,
    )


def solution(mesh):
    rows = P(("keys", "view"))
    wide = P(("keys", "view"), None)
    placed = (
        P(), rows, rows, rows, wide, rows, rows, wide, rows, rows, rows, wide, rows, rows, rows,
        wide, rows,
    )
    return jax.shard_map(
        shards, mesh=mesh, in_specs=placed, out_specs=wide, check_vma=False
    )
```

```python
import jax
import jax.numpy as jnp
from jax import lax
from jax.experimental import pallas as pl
from jax.experimental.pallas import tpu as pltpu
from jax.sharding import PartitionSpec as P

MESH = pl.DeviceIdType.MESH
F32, BF16, I32 = jnp.float32, jnp.bfloat16, jnp.int32
D = 256
KEYS_DEV = 512
GROUPS_DEV = 32
ROWS = 4096
DELTA = 1024
CAP = 64
OWNERS = 32
VIEWS = 4
LANES = 128
PEERS = 64
HALF = 2048
CHUNK = 512


def apart(code):
    return sum((0, 1, 2, 1)[d] for d in (code >> 4, (code >> 2) & 3, code & 3))


FAR_FIRST = sorted(range(PEERS), key=lambda code: (-apart(code), (code * 27) % PEERS))
OWNERS_MIXED = [11 * n % OWNERS for n in range(1, OWNERS)]
RANK = [FAR_FIRST.index(code) for code in range(PEERS)]


def iota(shape, dim):
    return lax.broadcasted_iota(I32, shape, dim)


def dot(a, b):
    return jnp.dot(a, b, preferred_element_type=F32)


def one_hot(rows, height, base, values=None):
    at = iota((height, LANES), 0)
    parts = []
    for n, row in enumerate(rows):
        value = 1.0 if values is None else values[n]
        parts.append(jnp.where(at == row - base, value, 0.0).astype(BF16))
    return jnp.concatenate(parts, axis=1)


def places(table, key_ref, count):
    keys = [key_ref[s : s + 1, :] for s in range(DELTA // LANES)]
    at = iota((LANES, LANES), 0)
    hits = jnp.concatenate(
        [jnp.where(at == (k >> 7), 1.0, 0.0).astype(BF16) for k in keys], axis=1
    )
    found = dot(table, hits)
    slots, owners, lives, marks = [], [], [], []
    lane = iota((1, LANES), 1)
    owner_at = iota((OWNERS, LANES), 0)
    for s, k in enumerate(keys):
        cut = slice(s * LANES, (s + 1) * LANES)
        value = found[:LANES, cut] * 128.0 + found[LANES:, cut]
        slot = jnp.sum(jnp.where(at == (k & 127), value, 0.0), axis=0, keepdims=True).astype(I32)
        live = lane + s * LANES < count
        owner = jnp.where(live, slot >> 9, -1)
        slots.append(slot & (KEYS_DEV - 1))
        owners.append(owner)
        lives.append(live)
        marks.append(jnp.where(owner_at == owner, 1.0, 0.0))
    stacked = jnp.concatenate(marks, axis=0).astype(BF16)
    col = iota((LANES, 2 * LANES), 1)
    before = jnp.where((iota((LANES, 2 * LANES), 0) < col) | (col >= LANES), 1.0, 0.0).astype(BF16)
    counts = dot(stacked, before)
    carry = jnp.zeros((OWNERS, LANES), F32)
    spots, ranks = [], []
    for s in range(len(keys)):
        cut = slice(s * OWNERS, (s + 1) * OWNERS)
        rank = jnp.sum(marks[s] * (counts[cut, :LANES] + carry), axis=0, keepdims=True).astype(I32)
        ranks.append(rank)
        spots.append(jnp.where(lives[s], owners[s] * CAP + rank, -1))
        carry = carry + counts[cut, LANES:]
    return slots, spots, marks, ranks


def by_place(marks, ranks, values):
    rank_at = iota((LANES, LANES), 0) & (CAP - 1)
    there = jnp.concatenate(
        [jnp.where(rank_at == rank, 1.0, 0.0).astype(BF16) for rank in ranks], axis=1
    )
    rows = jnp.concatenate(
        [
            jnp.concatenate([mark * v.astype(F32) for mark, v in zip(marks, value)], axis=1)
            for value in values
        ],
        axis=0,
    ).astype(BF16)
    return lax.dot_general(rows, there, (((1,), (1,)), ((), ())), preferred_element_type=F32)


def wait_bytes(ref, sem):
    pltpu.make_async_copy(ref, ref, sem).wait()


def kernel(
    key_slot_hbm, db_key_hbm, db_mult_hbm, db_count_hbm, db_hbm, b_slot_hbm, b_weight_hbm, b_hbm,
    da_key_hbm, da_group_hbm, da_mult_hbm, da_count_hbm, da_hbm, a_slot_hbm, a_weight_hbm,
    a_group_hbm, a_hbm,
    out,
    key_slot, db_key, db_mult, b_slot, b_weight, da_key, da_group, da_mult, a_slot, a_weight,
    a_group, da_count, db_count, da_rows, db_rows, b_rows, a_rows, spot_ref, sign_ref,
    db_send, da_send, db_info, da_info, db_recv, da_recv, db_info_recv, da_info_recv,
    part_b, quarter_b, got_b, full_b, part_db, quarter_db, got_db, full_db,
    pick, pick_d, table_a, table_w, terms, spots, near_send, near_recv, far_send, far_recv, own, chunk_sum, part_sum,
    spot_cols, a_turned, a_term,
    load_sems, sems, near_sems, part_sems, far_sems, planes,
):
    k, x = lax.axis_index("keys"), lax.axis_index("view")
    core = lax.rem(k, 2)
    partner = k + 1 - 2 * core
    y, z = k // 8, lax.rem(k // 2, 4)

    pairs = (
        (key_slot_hbm, key_slot), (db_key_hbm, db_key), (db_mult_hbm, db_mult),
        (db_count_hbm, db_count), (db_hbm, db_rows), (b_slot_hbm, b_slot),
        (b_weight_hbm, b_weight), (b_hbm, b_rows), (da_key_hbm, da_key),
        (da_group_hbm, da_group), (da_mult_hbm, da_mult), (da_count_hbm, da_count),
        (da_hbm, da_rows), (a_slot_hbm, a_slot), (a_weight_hbm, a_weight),
        (a_group_hbm, a_group), (a_hbm, a_rows),
    )
    loads = [
        pltpu.make_async_copy(src, dst, load_sems.at[n]) for n, (src, dst) in enumerate(pairs)
    ]
    for n in range(4):
        loads[n].start()

    def peer(code):
        to_y, to_z = lax.rem(y + (code >> 4), 4), lax.rem(z + ((code >> 2) & 3), 4)
        return {"keys": (to_y * 4 + to_z) * 2 + core, "view": lax.rem(x + (code & 3), VIEWS)}

    def send(src, dst, sem_s, sem_r, device):
        return pltpu.make_async_remote_copy(
            src_ref=src, dst_ref=dst, send_sem=sem_s, recv_sem=sem_r, device_id=device,
            device_id_type=MESH,
        )

    barrier = pltpu.get_barrier_semaphore()

    def greet(j, carry):
        to = {"keys": lax.rem(k + j, OWNERS), "view": x}
        pl.semaphore_signal(barrier, inc=1, device_id=to, device_id_type=MESH)
        return carry

    with jax.named_scope("greet"):
        lax.fori_loop(1, OWNERS, greet, 0)
        for j in range(1, VIEWS):
            to = {"keys": k, "view": lax.rem(x + j, VIEWS)}
            pl.semaphore_signal(barrier, inc=1, device_id=to, device_id_type=MESH)
        for n in range(4, len(loads)):
            loads[n].start()

    with jax.named_scope("lookup_b"):
        for n in range(4):
            loads[n].wait()
        whole = key_slot[...]
        high = (whole >> 7).astype(F32).T
        low = (whole & 127).astype(F32).T
        table = jnp.concatenate([high, low], axis=0).astype(BF16)

        def look_up(r, key_ref, mult_ref, count_ref):
            slots, found, marks, ranks = places(table, key_ref, count_ref[0])
            for s in range(8):
                spot_ref[8 * r + s : 8 * r + s + 1, :] = found[s]
                sign_ref[8 * r + s : 8 * r + s + 1, :] = mult_ref[s : s + 1, :].astype(F32)
            return slots, marks, ranks

        slots_b, marks_b, ranks_b = look_up(0, db_key, db_mult, db_count)
        note = by_place(
            marks_b, ranks_b, [[v >> 4 for v in slots_b], [v & 15 for v in slots_b]]
        )
        note = (note[:OWNERS] * 16.0 + note[OWNERS:]).astype(I32)
        for n in range(OWNERS):
            db_info[n] = note[n : n + 1, :]

    def owner_of(code):
        to_y, to_z = lax.rem(y + code // 8, 4), lax.rem(z + (code // 2) % 4, 4)
        return (to_y * 4 + to_z) * 2 + lax.rem(core + code % 2, 2)

    def packed(r, i, rows):
        spots = [spot_ref[8 * r + s : 8 * r + s + 1, :] for s in range(8)]
        signs = [sign_ref[8 * r + s : 8 * r + s + 1, :] for s in range(8)]
        return dot(one_hot(spots, 512, 512 * i, signs), rows[...]).astype(BF16)

    loads[4].wait()

    def pack_b(i, carry):
        blocks = packed(0, i, db_rows).reshape(8, CAP, D)
        for h in range(2):
            db_send[h, pl.ds(8 * i, 8)] = blocks[:, :, h * LANES : (h + 1) * LANES]
        return carry

    with jax.named_scope("pack_b"):
        lax.fori_loop(0, 4, pack_b, 0)

    with jax.named_scope("barrier"):
        pl.semaphore_wait(barrier, OWNERS - 1 + VIEWS - 1)

    with jax.named_scope("send_b"):
        for code in OWNERS_MIXED:
            n = owner_of(code)
            to = {"keys": n, "view": x}
            send(db_info.at[n], db_info_recv.at[code], sems.at[0], sems.at[1], to).start()
            send(db_send.at[0, n], db_recv.at[0, code], sems.at[2], sems.at[3], to).start()
        for code in OWNERS_MIXED:
            n = owner_of(code)
            to = {"keys": n, "view": x}
            send(db_send.at[1, n], db_recv.at[1, code], sems.at[4], sems.at[5], to).start()
        for j in range(1, VIEWS):
            to = {"keys": k, "view": lax.rem(x + j, VIEWS)}
            pl.semaphore_signal(planes, inc=1, device_id=to, device_id_type=MESH)
    db_info_recv[0] = db_info[k]
    db_recv[0, 0] = db_send[0, k]
    db_recv[1, 0] = db_send[1, k]

    def eighth(at, part):
        return pl.ds(pl.multiple_of(at * 128 + part * 64, 64), 64)

    def quarter(at):
        return pl.ds(pl.multiple_of(at * 128, 128), 128)

    def across(part, got, s):
        for j in range(1, VIEWS):
            to = lax.rem(x + j, VIEWS)
            send(
                part.at[quarter(to)], got.at[j - 1], sems.at[s], sems.at[s + 1],
                {"keys": k, "view": to},
            ).start()

    def all_quarters(mine, full, s):
        for j in range(1, VIEWS):
            to = lax.rem(x + j, VIEWS)
            send(
                mine, full.at[quarter(x)], sems.at[s], sems.at[s + 1], {"keys": k, "view": to}
            ).start()

    for n in (5, 6, 7):
        loads[n].wait()
    with jax.named_scope("sum_b"):
        for m in range(2):
            acc = jnp.zeros((256, D), F32)
            for p in range(8):
                rows = [b_slot[4 * p + s : 4 * p + s + 1, :] for s in range(4)]
                values = [b_weight[4 * p + s : 4 * p + s + 1, :].astype(F32) for s in range(4)]
                hits = one_hot(rows, 256, 256 * m, values)
                acc = acc + dot(hits, b_rows[512 * p : 512 * (p + 1), :])
            part_b[256 * m : 256 * (m + 1), :] = acc
        across(part_b, got_b, 8)

    with jax.named_scope("lookup_a"):
        for n in range(8, 12):
            loads[n].wait()
        slots_a, marks_a, ranks_a = look_up(1, da_key, da_mult, da_count)
        groups = [da_group[s : s + 1, :] for s in range(8)]
        note = by_place(
            marks_a,
            ranks_a,
            [
                [v >> 4 for v in slots_a],
                [v & 15 for v in slots_a],
                [v >> 6 for v in groups],
                [v & 63 for v in groups],
            ],
        )
        slot_note = (note[:OWNERS] * 16.0 + note[OWNERS : 2 * OWNERS]).astype(I32)
        group_note = (note[2 * OWNERS : 3 * OWNERS] * 64.0 + note[3 * OWNERS :]).astype(I32)
        for n in range(OWNERS):
            da_info[n] = jnp.concatenate([slot_note[n : n + 1, :], group_note[n : n + 1, :]], axis=0)
    loads[12].wait()

    def pack_a(i, carry):
        da_send[pl.ds(8 * i, 8)] = packed(1, i, da_rows).reshape(8, CAP, D)
        return carry

    with jax.named_scope("pack_a"):
        lax.fori_loop(0, 4, pack_a, 0)

    for code in OWNERS_MIXED:
        n = owner_of(code)
        to = {"keys": n, "view": x}
        send(da_info.at[n], da_info_recv.at[code], sems.at[6], sems.at[7], to).start()
    da_info_recv[0] = da_info[k]
    da_recv[0] = da_send[k]

    left = iota((1, LANES), 1) < CAP

    def pair(ref, row, n):
        return jnp.where(left, ref[2 * n, row : row + 1, :], ref[2 * n + 1, row : row + 1, :])

    def sum_db(h):
        for m in range(2):
            acc = jnp.zeros((256, LANES), F32)
            for p in range(4):
                rows = [pair(db_info_recv, 0, 4 * p + s) for s in range(4)]
                blocks = db_recv[h, 8 * p : 8 * (p + 1)].reshape(512, LANES)
                acc = acc + dot(one_hot(rows, 256, 256 * m), blocks)
            part_db[h, 256 * m : 256 * (m + 1), :] = acc

    def finish_quarter(h):
        quarter_db[h] = part_db[h, quarter(x), :] + got_db[h, 0] + got_db[h, 1] + got_db[h, 2]
        all_quarters(quarter_db.at[h], full_db.at[h], 16 + 4 * h)
        full_db[h, quarter(x), :] = quarter_db[h]

    at_lane = iota((LANES, LANES), 1)

    def place(group):
        to_y, to_z, to_x = group >> 10, (group >> 8) & 3, (group >> 5) & 3
        code = ((to_y - y) & 3) * 16 + ((to_z - z) & 3) * 4 + ((to_x - x) & 3)
        rank = jnp.zeros_like(code)
        for n in range(PEERS):
            rank = jnp.where(code == n, RANK[n], rank)
        other = ((group >> 7) & 1) ^ core
        return other * HALF + rank * GROUPS_DEV + (group & 31)

    for n in range(13, 17):
        loads[n].wait()
    with jax.named_scope("pick"):
        spots[0:32, :] = place(a_group[...])

        def pick_block(j, carry):
            at = pl.ds(pl.multiple_of(j * LANES, LANES), LANES)
            value = a_weight[pl.ds(j, 1), :].astype(F32)
            pick[:, at] = one_hot([a_slot[pl.ds(j, 1), :]], KEYS_DEV, 0, [value])
            row = jnp.broadcast_to(spots[pl.ds(j, 1), :].astype(F32), (LANES, LANES))
            spot_cols[at, :] = row.T.astype(I32) - at_lane
            turned = a_rows[at, :].astype(F32).T.astype(BF16)
            for h in range(2):
                a_turned[h, :, at] = turned[h * LANES : (h + 1) * LANES, :]
            return carry

        lax.fori_loop(0, 32, pick_block, 0)

    with jax.named_scope("wait_db0"):
        wait_bytes(db_info_recv.at[1:OWNERS], sems.at[1])
        wait_bytes(db_recv.at[0, 1:OWNERS], sems.at[3])
    sum_db(0)
    across(part_db.at[0], got_db.at[0], 14)

    with jax.named_scope("wait_b"):
        wait_bytes(got_b, sems.at[9])
    whole_b = part_b[quarter(x), :] + got_b[0] + got_b[1] + got_b[2]
    for h in range(2):
        quarter_b[h] = whole_b[:, h * LANES : (h + 1) * LANES]
        full_b[h, quarter(x), :] = quarter_b[h]

    with jax.named_scope("wait_db1"):
        wait_bytes(db_recv.at[1, 1:OWNERS], sems.at[5])
    for code in OWNERS_MIXED:
        n = owner_of(code)
        to = {"keys": n, "view": x}
        send(da_send.at[n], da_recv.at[code], sems.at[12], sems.at[13], to).start()
    sum_db(1)
    for part in range(2):
        for j in range(1, VIEWS):
            to = lax.rem(x + j, VIEWS)
            send(
                part_db.at[1, eighth(to, part)], got_db.at[1, j - 1, 64 * part : 64 * part + 64],
                part_sems.at[part, 0], part_sems.at[part, 1], {"keys": k, "view": to},
            ).start()

    with jax.named_scope("wait_rs0"):
        wait_bytes(got_db.at[0], sems.at[15])
    finish_quarter(0)


    with jax.named_scope("wait_da_info"):
        wait_bytes(da_info_recv.at[1:OWNERS], sems.at[7])
    with jax.named_scope("pick_d"):
        groups_d = jnp.concatenate([pair(da_info_recv, 1, n) for n in range(16)], axis=0)
        spots[32:48, :] = place(groups_d)
        for n in range(16):
            cols = jnp.broadcast_to(
                pair(da_info_recv, 0, n).astype(F32), (LANES, LANES)
            ).T.astype(I32)
            for q in range(4):
                pick_d[n * LANES : (n + 1) * LANES, q * LANES : (q + 1) * LANES] = jnp.where(
                    at_lane + q * LANES == cols, 1.0, 0.0
                ).astype(BF16)

    def split(value):
        top = value.astype(BF16)
        return jnp.concatenate([top, (value - top.astype(F32)).astype(BF16)], axis=1)

    def a_terms(h):
        flat = full_db[h].T
        top = flat.astype(BF16)
        table_a[...] = jnp.concatenate([top, (flat - top.astype(F32)).astype(BF16)], axis=0)

        def block(j, carry):
            at = pl.ds(pl.multiple_of(j * 2048, 2048), 2048)
            both = dot(table_a[...], pick[:, at])
            value = (both[:LANES] + both[LANES:]) * a_turned[h, :, at].astype(F32)
            a_term[h, :, at] = value.astype(BF16)
            return carry

        lax.fori_loop(0, 2, block, 0)

    def pick_base(t, bases):
        base = 0
        for n, value in enumerate(bases):
            base = jnp.where(t == n, value, base)
        return base

    def a_sum(h, base, width):
        acc = jnp.zeros((LANES, width), F32)
        for p in range(16):
            at = slice(256 * p, 256 * (p + 1))
            cols = spot_cols[at, :] - base
            hits = jnp.concatenate(
                [
                    jnp.where(cols == q * LANES, 1.0, 0.0).astype(BF16)
                    for q in range(width // LANES)
                ],
                axis=1,
            )
            acc = acc + dot(a_term[h, :, at], hits)
        return acc.T

    def a_sums(h, bases, width=1024):
        def block(t, carry):
            base = pl.multiple_of(pick_base(t, bases), width)
            part_sum[pl.ds(base, width), h * LANES : (h + 1) * LANES] = a_sum(h, base, width)
            return carry

        lax.fori_loop(0, len(bases), block, 0)

    for part in range(2):
        cut = slice(64 * part, 64 * part + 64)
        with jax.named_scope("wait_rs1"):
            wait_bytes(got_db.at[1, :, cut], part_sems.at[part, 1])
        quarter_db[1, cut] = (
            part_db[1, eighth(x, part), :]
            + got_db[1, 0, cut]
            + got_db[1, 1, cut]
            + got_db[1, 2, cut]
        )
        for j in range(1, VIEWS):
            to = lax.rem(x + j, VIEWS)
            send(
                quarter_db.at[1, cut], full_db.at[1, eighth(x, part)], sems.at[20], sems.at[21],
                {"keys": k, "view": to},
            ).start()
        full_db[1, eighth(x, part), :] = quarter_db[1, cut]

    for h in range(2):
        all_quarters(quarter_b.at[h], full_b.at[h], 10 + 14 * h)
    with jax.named_scope("wait_ag0"):
        wait_bytes(full_db.at[0, 0:384], sems.at[17])
    with jax.named_scope("a_terms0"):
        a_terms(0)
    with jax.named_scope("a_sums0b"):
        a_sums(0, [HALF, 0])
    with jax.named_scope("wait_ag1"):
        wait_bytes(full_db.at[1, 0:384], sems.at[21])
    with jax.named_scope("a_terms1"):
        a_terms(1)
    with jax.named_scope("a_sums1a"):
        a_sums(1, [HALF])

    with jax.named_scope("wait_ag_b"):
        wait_bytes(full_b.at[0, 0:384], sems.at[11])
        wait_bytes(full_b.at[1, 0:384], sems.at[25])
    for h in range(2):
        table_w[h] = split(full_db[h] + full_b[h])

    with jax.named_scope("wait_da"):
        wait_bytes(da_recv.at[1:OWNERS], sems.at[13])

    def d_block(j, carry):
        at = pl.ds(pl.multiple_of(j * 1024, 1024), 1024)
        rows = da_recv[pl.ds(16 * j, 16)].reshape(1024, D).astype(F32)
        for h in range(2):
            both = dot(pick_d[at, :], table_w[h])
            value = (both[:, :LANES] + both[:, LANES:]) * rows[:, h * LANES : (h + 1) * LANES]
            terms[at, h * LANES : (h + 1) * LANES] = value.astype(BF16)
        return carry

    with jax.named_scope("d_terms"):
        lax.fori_loop(0, 2, d_block, 0)

    def to_partner(c):
        rows = slice(c * CHUNK, (c + 1) * CHUNK)
        near_send[rows] = chunk_sum[...]
        send(
            near_send.at[rows], near_recv.at[rows], near_sems.at[0, c], near_sems.at[1, c],
            {"keys": partner, "view": x},
        ).start()

    def to_groups(c):
        rows = slice(c * CHUNK, (c + 1) * CHUNK)
        blocks = range(c * CHUNK // GROUPS_DEV, (c + 1) * CHUNK // GROUPS_DEV)
        wait_bytes(near_recv.at[rows], near_sems.at[1, c])
        acc = chunk_sum[...] + near_recv[rows]
        if blocks.stop == PEERS:
            own[...] = acc[CHUNK - GROUPS_DEV :, :]
        far_send[blocks.start : blocks.stop] = acc.astype(BF16).reshape(
            len(blocks), GROUPS_DEV, D
        )
        if c == 0:
            pl.semaphore_wait(planes, VIEWS - 1)
        for m in blocks:
            code = FAR_FIRST[m]
            if code:
                send(
                    far_send.at[m], far_recv.at[m], sems.at[22], far_sems.at[c], peer(code)
                ).start()

    def d_sum(base):
        acc = jnp.zeros((CHUNK, D), F32)
        for p in range(4):
            rows = [spots[32 + 4 * p + s : 33 + 4 * p + s, :] for s in range(4)]
            acc = acc + dot(one_hot(rows, CHUNK, base), terms[512 * p : 512 * (p + 1), :])
        return acc

    def sums(steps, begun):
        def block(t, carry):
            base = pick_base(t, [other * HALF + c * CHUNK for other, c in steps])
            base = pl.multiple_of(base, CHUNK)
            at = pl.ds(base, CHUNK)
            if begun:
                chunk_sum[...] = d_sum(base) + part_sum[at, :]
            else:
                turned = a_sum(1, base, CHUNK)
                acc = d_sum(base)
                chunk_sum[:, :LANES] = acc[:, :LANES] + part_sum[at, :LANES]
                chunk_sum[:, LANES:] = acc[:, LANES:] + turned
            for n, (other, c) in enumerate(steps):
                pl.when(t == n)(lambda other=other, c=c: (to_partner if other else to_groups)(c))
            return carry

        lax.fori_loop(0, len(steps), block, 0)

    with jax.named_scope("sums1"):
        sums([(1, 0), (1, 1)], True)
    with jax.named_scope("sums2"):
        sums([(0, 0), (0, 1)], False)
    with jax.named_scope("sums3"):
        a_sums(0, [HALF + 1024])
        sums([(1, 2), (1, 3)], False)
    with jax.named_scope("sums4"):
        a_sums(0, [1024])
        sums([(0, 2), (0, 3)], False)

    total = own[...]
    for c in range(HALF // CHUNK):
        first, stop = c * CHUNK // GROUPS_DEV, min((c + 1) * CHUNK // GROUPS_DEV, PEERS - 1)
        with jax.named_scope("wait_far" if stop == PEERS - 1 else "arrive"):
            wait_bytes(far_recv.at[first:stop], far_sems.at[c])
        for m in range(first, stop):
            total = total + far_recv[m].astype(F32)
    out[...] = total

    wait_bytes(db_info.at[1:OWNERS], sems.at[0])
    wait_bytes(db_send.at[0, 1:OWNERS], sems.at[2])
    wait_bytes(db_send.at[1, 1:OWNERS], sems.at[4])
    wait_bytes(da_info.at[1:OWNERS], sems.at[6])
    wait_bytes(part_b.at[0:384], sems.at[8])
    wait_bytes(full_b.at[0, 0:384], sems.at[10])
    wait_bytes(full_b.at[1, 0:384], sems.at[24])
    wait_bytes(da_send.at[1:OWNERS], sems.at[12])
    for h in range(2):
        wait_bytes(part_db.at[h, 0:384], sems.at[16 + 4 * h])
        wait_bytes(got_db.at[1, :, 0:64], part_sems.at[h, 0])
    wait_bytes(part_db.at[0, 0:384], sems.at[14])
    wait_bytes(far_send.at[0 : PEERS - 1], sems.at[22])
    for c in range(HALF // CHUNK):
        wait_bytes(near_send.at[c * CHUNK : (c + 1) * CHUNK], near_sems.at[0, c])


def shards(
    key_slot, a_slot, a_group, a_weight, a_payload, b_slot, b_weight, b_payload, da_key, da_group,
    da_mult, da_payload, da_count, db_key, db_mult, db_payload, db_count,
):
    vmem = pl.BlockSpec(memory_space=pltpu.VMEM)
    hbm = pl.BlockSpec(memory_space=pl.ANY)

    def lanes(v):
        return v.reshape(-1, LANES)

    def held(*shape, dtype=F32):
        return pltpu.VMEM(shape, dtype)

    return pl.pallas_call(
        kernel,
        out_shape=jax.ShapeDtypeStruct((GROUPS_DEV, D), F32),
        in_specs=[hbm] * 17,
        out_specs=vmem,
        scratch_shapes=[
            held(LANES, LANES, dtype=I32),
            held(8, LANES, dtype=I32),
            held(8, LANES, dtype=I32),
            held(32, LANES, dtype=I32),
            held(32, LANES, dtype=I32),
            held(8, LANES, dtype=I32),
            held(8, LANES, dtype=I32),
            held(8, LANES, dtype=I32),
            held(32, LANES, dtype=I32),
            held(32, LANES, dtype=I32),
            held(32, LANES, dtype=I32),
            pltpu.SMEM((1,), I32),
            pltpu.SMEM((1,), I32),
            held(DELTA, D, dtype=BF16),
            held(DELTA, D, dtype=BF16),
            held(ROWS, D, dtype=BF16),
            held(ROWS, D, dtype=BF16),
            held(16, LANES, dtype=I32),
            held(16, LANES),
            held(2, OWNERS, CAP, LANES, dtype=BF16),
            held(OWNERS, CAP, D, dtype=BF16),
            held(OWNERS, 1, LANES, dtype=I32),
            held(OWNERS, 2, LANES, dtype=I32),
            held(2, OWNERS, CAP, LANES, dtype=BF16),
            held(OWNERS, CAP, D, dtype=BF16),
            held(OWNERS, 1, LANES, dtype=I32),
            held(OWNERS, 2, LANES, dtype=I32),
            held(KEYS_DEV, D),
            held(2, 128, LANES),
            held(3, 128, D),
            held(2, KEYS_DEV, LANES),
            held(2, KEYS_DEV, LANES),
            held(2, 128, LANES),
            held(2, 3, 128, LANES),
            held(2, KEYS_DEV, LANES),
            held(KEYS_DEV, ROWS, dtype=BF16),
            held(OWNERS * CAP, KEYS_DEV, dtype=BF16),
            held(D, KEYS_DEV, dtype=BF16),
            held(2, KEYS_DEV, D, dtype=BF16),
            held(OWNERS * CAP, D, dtype=BF16),
            held(48, LANES, dtype=I32),
            held(HALF, D),
            held(HALF, D),
            held(PEERS, GROUPS_DEV, D, dtype=BF16),
            held(PEERS, GROUPS_DEV, D, dtype=BF16),
            held(GROUPS_DEV, D),
            held(CHUNK, D),
            held(PEERS * 2 * GROUPS_DEV, D),
            held(ROWS, LANES, dtype=I32),
            held(2, LANES, ROWS, dtype=BF16),
            held(2, LANES, ROWS, dtype=BF16),
            pltpu.SemaphoreType.DMA((17,)),
            pltpu.SemaphoreType.DMA((26,)),
            pltpu.SemaphoreType.DMA((2, HALF // CHUNK)),
            pltpu.SemaphoreType.DMA((2, 2)),
            pltpu.SemaphoreType.DMA((HALF // CHUNK,)),
            pltpu.SemaphoreType.REGULAR,
        ],
        compiler_params=pltpu.CompilerParams(
            collective_id=0, has_side_effects=True, vmem_limit_bytes=56 * 1024 * 1024
        ),
    )(
        lanes(key_slot), lanes(db_key), lanes(db_mult), db_count, db_payload, lanes(b_slot),
        lanes(b_weight), b_payload, lanes(da_key), lanes(da_group), lanes(da_mult), da_count,
        da_payload, lanes(a_slot), lanes(a_weight), lanes(a_group), a_payload,
    )


def solution(mesh):
    rows = P(("keys", "view"))
    wide = P(("keys", "view"), None)
    placed = (
        P(), rows, rows, rows, wide, rows, rows, wide, rows, rows, rows, wide, rows, rows, rows,
        wide, rows,
    )
    return jax.shard_map(
        shards, mesh=mesh, in_specs=placed, out_specs=wide, check_vma=False
    )
```
